32 devices in a mesh: seq: 16 (over z, y, x), head: 2 (over core).
Axes of the slice: x: 2, y: 2, z: 4, core: 2. Of those that a mesh axis runs over, the one named last changes fastest.
Arguments:
- queries: bfloat16 [2048, 32, 128], P('seq', 'head'), may hold values from -6 to 6
- key_vectors: bfloat16 [2048, 32, 128], P('seq', 'head'), may hold values from -6 to 6
- values: bfloat16 [2048, 32, 128], P('seq', 'head'), may hold values from -6 to 6
- out_grad: bfloat16 [2048, 32, 128], P('seq', 'head'), may hold values from -6 to 6
- hidden_in: bfloat16 [2048, 2048], P('seq'), may hold values from -6 to 6
- decay_weight: bfloat16 [2048, 32], P(None, 'head'), may hold values from -0.125 to 0.125
- write_weight: bfloat16 [2048, 32], P(None, 'head'), may hold values from -0.125 to 0.125
- decay_bias: float32 [32], P('head'), may hold values from -2 to 2
- decay_log: float32 [32], P('head'), may hold values from -11 to -2
- write_bias: float32 [32], P('head'), may hold values from -9 to 0
- start_state: float32 [16, 32, 128, 128], P('seq', 'head'), may hold values from -4 to 4
Outputs:
- grad_queries: bfloat16 [2048, 32, 128], P('seq', 'head')
- grad_keys: bfloat16 [2048, 32, 128], P('seq', 'head')
- grad_values: bfloat16 [2048, 32, 128], P('seq', 'head')
- grad_hidden: bfloat16 [2048, 2048], P('seq', 'head')
- grad_decay_weight: float32 [2048, 32], P(None, 'head')
- grad_write_weight: float32 [2048, 32], P(None, 'head')
The draws below stay inside these ranges and needn't reach their ends.
All inputs are finite; a program needn't handle non-finite values.
Results may differ from the reference program's by a relative error of at most 0.014.
Values may be sent and summed in bfloat16 or wider, within the bound.
A program may use at most 128 MiB of HBM per device.

```python
from functools import partial
import jax
import jax.numpy as jnp
from jax import lax

D = 2048
HEADS = 32
DK = 128
DV = 128
TOK_DEV = 128
BLOCKS = 16
TOKENS = 2048


def block_scale(own_key, extent, shards, least, top_value):
    def one(axis_at, blocks):
        draws = jax.random.uniform(jax.random.fold_in(jax.random.fold_in(own_key, 6), axis_at), (blocks,), jnp.float32, least / len(shards), top_value / len(shards))
        return jnp.repeat(jnp.exp(draws), extent[axis_at] // blocks).reshape((-1,) + (1,) * (len(extent) - axis_at - 1))

    level = one(*shards[0])
    for cut in shards[1:]:
        level = level * one(*cut)
    return level


def scatter_about(own_key, extent, scale, most, split=(), held_as=jnp.bfloat16):
    loudness = block_scale(own_key, extent, split, -0.22, 0.18) if split else 1.0
    array = jax.random.normal(own_key, extent, jnp.float32) * scale * loudness
    return jnp.minimum(jnp.maximum(array, -most), most).astype(held_as)


def setup_inputs(seed: int = 0) -> dict:
    key_of = jax.random.split(jax.random.key(seed), 12)
    return {
        "queries": scatter_about(key_of[0], (TOKENS, HEADS, DK), 1.0, 6.0, ((0, 16), (1, 2))),
        "key_vectors": scatter_about(key_of[1], (TOKENS, HEADS, DK), 1.0, 6.0, ((0, 16), (1, 2))),
        "values": scatter_about(key_of[2], (TOKENS, HEADS, DV), 1.0, 6.0, ((0, 16), (1, 2))),
        "out_grad": scatter_about(key_of[3], (TOKENS, HEADS, DV), 1.0, 6.0, ((0, 16), (1, 2))),
        "hidden_in": scatter_about(key_of[4], (TOKENS, D), 1.0, 6.0, ((0, 16),)),
        "decay_weight": scatter_about(key_of[5], (D, HEADS), D ** -0.5, 0.125, ((1, 2),)),
        "write_weight": scatter_about(key_of[6], (D, HEADS), D ** -0.5, 0.125, ((1, 2),)),
        "decay_bias": jnp.clip(jax.random.uniform(key_of[7], (HEADS,), jnp.float32, -2.0, 2.0) * block_scale(key_of[7], (HEADS,), ((0, 2),), -0.4, 0.0), -2.0, 2.0),
        "decay_log": jnp.clip(-11.0 + 9.0 * jax.random.uniform(key_of[8], (HEADS,), jnp.float32) ** block_scale(key_of[8], (HEADS,), ((0, 2),), -0.2, 0.2), -11.0, -2.0),
        "write_bias": jnp.clip(-9.0 + 9.0 * jax.random.uniform(key_of[9], (HEADS,), jnp.float32) ** block_scale(key_of[9], (HEADS,), ((0, 2),), -0.2, 0.2), -9.0, 0.0),
        "start_state": scatter_about(key_of[10], (BLOCKS, HEADS, DK, DV), 0.5, 4.0, ((0, 16), (1, 2)), jnp.float32),
    }


EPSILON = 1e-06
PRECISION_MAXIMUM = lax.Precision.HIGHEST

def block_forward(decay_log, decay_bias, write_bias, queries, key_vectors, values, decay_logit, write_logit, initial_state):
    normalized_queries = queries * lax.rsqrt(lax.optimization_barrier(jnp.sum(queries * queries, axis=-1, keepdims=True)) + EPSILON)
    normalized_keys = key_vectors * lax.rsqrt(lax.optimization_barrier(jnp.sum(key_vectors * key_vectors, axis=-1, keepdims=True)) + EPSILON)
    write_rate = jax.nn.sigmoid(write_logit + write_bias)
    log_decay = -jnp.exp(decay_log) * jax.nn.softplus(decay_logit + decay_bias)
    log_prefix = jnp.cumsum(log_decay, axis=0).T
    block_size = queries.shape[0]
    positions = jnp.arange(block_size, dtype=jnp.int32)
    lower_mask = positions[:, None] >= positions[None, :]
    strict_mask = positions[:, None] > positions[None, :]
    log_gaps = jnp.where(lower_mask, log_prefix[:, :, None] - log_prefix[:, None, :], 0.0)
    decay_ratio = jnp.where(lower_mask, jnp.exp(log_gaps), 0.0)
    key_gram = jnp.einsum('ihk,jhk->hij', normalized_keys, normalized_keys, precision=PRECISION_MAXIMUM)
    coupling = jnp.where(strict_mask, write_rate.T[:, :, None] * decay_ratio * key_gram, 0.0)
    unit_lower = coupling + jnp.eye(block_size, dtype=coupling.dtype)
    cumulative_decay = jnp.exp(log_prefix)
    keys_against_state = jnp.einsum('dlu,lux->ldx', normalized_keys, initial_state, precision=PRECISION_MAXIMUM)
    right_side = write_rate.T[:, :, None] * (jnp.swapaxes(values, 0, 1) - cumulative_decay[:, :, None] * keys_against_state)
    value_updates = jax.scipy.linalg.solve_triangular(unit_lower, right_side, lower=True, unit_diagonal=True)
    query_keys = decay_ratio * jnp.einsum('ihk,jhk->hij', normalized_queries, normalized_keys, precision=PRECISION_MAXIMUM)
    layer_outputs = cumulative_decay[:, :, None] * jnp.einsum('dlu,lux->ldx', normalized_queries, initial_state, precision=PRECISION_MAXIMUM)
    layer_outputs = layer_outputs + jnp.einsum('hij,hjv->hiv', query_keys, value_updates, precision=PRECISION_MAXIMUM)
    final_decay_weights = decay_ratio[:, -1, :]
    final_state = cumulative_decay[:, -1][:, None, None] * initial_state + jnp.einsum('zg,gzi,zgq->ziq', final_decay_weights, normalized_keys, value_updates, precision=PRECISION_MAXIMUM)
    return (jnp.swapaxes(layer_outputs, 0, 1), final_state)

def reference(queries, key_vectors, values, out_grad, hidden_in, decay_weight, write_weight, decay_bias, decay_log, write_bias, start_state):
    decay_logit = jnp.dot(hidden_in.astype(jnp.float32), decay_weight.astype(jnp.float32), preferred_element_type=jnp.float32)
    write_logit = jnp.dot(hidden_in.astype(jnp.float32), write_weight.astype(jnp.float32), preferred_element_type=jnp.float32)
    head_count = queries.shape[1]

    def blocked(source):
        return source.astype(jnp.float32).reshape((BLOCKS, TOK_DEV) + source.shape[1:])
    inputs = (blocked(queries), blocked(key_vectors), blocked(values), blocked(out_grad), blocked(decay_logit), blocked(write_logit), start_state)
    forward = partial(block_forward, decay_log, decay_bias, write_bias)

    def backward_block(carried, pieces):
        query_rows, key_rows, value_rows, grad_rows, decay_rows, write_rows, initial_state = pieces
        primal, pullback = jax.vjp(forward, query_rows, key_rows, value_rows, decay_rows, write_rows, initial_state)
        gradients = pullback((grad_rows, carried))
        return (gradients[5], gradients[:5])
    carried_init = jnp.zeros((head_count, DK, DV), jnp.float32)
    _, gradients = lax.scan(backward_block, carried_init, inputs, reverse=True)

    def joined(source):
        return source.reshape((TOKENS,) + source.shape[2:])
    grad_queries = joined(gradients[0]).astype(jnp.bfloat16)
    grad_keys = joined(gradients[1]).astype(jnp.bfloat16)
    grad_values = joined(gradients[2]).astype(jnp.bfloat16)
    decay_grads = joined(gradients[3]).astype(jnp.bfloat16)
    write_grads = joined(gradients[4]).astype(jnp.bfloat16)
    grad_decay_weight = jnp.dot(hidden_in.T.astype(jnp.float32), decay_grads.astype(jnp.float32), preferred_element_type=jnp.float32)
    grad_write_weight = jnp.dot(hidden_in.T.astype(jnp.float32), write_grads.astype(jnp.float32), preferred_element_type=jnp.float32)
    grad_hidden = jnp.dot(decay_grads.astype(jnp.float32), decay_weight.T.astype(jnp.float32), preferred_element_type=jnp.float32) + jnp.dot(write_grads.astype(jnp.float32), write_weight.T.astype(jnp.float32), preferred_element_type=jnp.float32)
    return (grad_queries, grad_keys, grad_values, grad_hidden.astype(jnp.bfloat16), grad_decay_weight, grad_write_weight)
```

```python
from functools import partial

import jax
import jax.numpy as jnp
from jax import lax
from jax.experimental import pallas as pl
from jax.experimental.pallas import tpu as pltpu
from jax.sharding import PartitionSpec as P

EPSILON = 1e-06
HI = lax.Precision.HIGHEST
F32 = jnp.float32
BF = jnp.bfloat16


def mm(a, b, ca=1, cb=0):
    return lax.dot_general(
        a.astype(BF), b.astype(BF), (((ca,), (cb,)), ((), ())), preferred_element_type=F32
    )


def unit(x):
    r = lax.rsqrt(jnp.sum(x * x, axis=1, keepdims=True) + EPSILON)
    return x * r, r


def unit_back(d, n, r):
    return r * (d - n * jnp.sum(n * d, axis=1, keepdims=True))


def indices(c):
    row = lax.broadcasted_iota(jnp.int32, (c, c), 0)
    col = lax.broadcasted_iota(jnp.int32, (c, c), 1)
    return row, col


def inverses(couplings):
    c = couplings[0].shape[0]
    row, col = indices(c)
    invs = [
        jnp.where(row == col, 1.0, jnp.where((row ^ col) == 1, -a, 0.0)) for a in couplings
    ]
    level = 1
    while (2 << level) <= c:
        near = ((row >> level) ^ (col >> level)) == 1
        halves = [mm(x, jnp.where(near, a, 0.0)) for x, a in zip(invs, couplings)]
        invs = [x - mm(y, x) for x, y in zip(invs, halves)]
        level += 1
    return invs


def decays(rows):
    c = rows.shape[1]
    cols = rows.T
    g_col, beta = cols[:, 0:1], cols[:, 1:2]
    g_row = rows[0:1, :]
    g_last = g_row[:, c - 1 : c]
    return g_col, g_row, g_last, beta, jnp.exp(g_col), jnp.exp(g_last - g_col)


def local_first(q, k, rows):
    c = q.shape[0]
    row, col = indices(c)
    g_col, g_row, g_last, beta, cd, to_end = decays(rows)
    lower = row >= col
    gamma = jnp.where(lower, jnp.exp(jnp.where(lower, g_col - g_row, 0.0)), 0.0)
    gs = jnp.where(row > col, gamma, 0.0)
    qn, _ = unit(q.astype(F32))
    kn, _ = unit(k.astype(F32))
    kb = kn.astype(BF)
    grams = mm(jnp.concatenate([qn.astype(BF), kb], axis=0), kb, 1, 1)
    p = gamma * grams[:c]
    gram = gs * grams[c:]
    return qn, kn, p, gram, gs, beta * gram, beta, cd, to_end, jnp.exp(g_last)


def local_map(do, inv, first):
    qn, kn, p, gram, gs, a, beta, cd, to_end, last = first
    c = qn.shape[0]
    ib = inv.astype(BF)
    ptdo = mm(p, do, 0, 0)
    both = mm(ib, jnp.concatenate([ptdo.astype(BF), (to_end * kn).astype(BF)], axis=1), 0, 0)
    dv = do.shape[1]
    bck = ((beta * cd) * kn).astype(BF)
    prod = mm(bck, both, 0, 0)
    off = mm(cd * qn, do, 0, 0) - prod[:, :dv]
    return ib, both[:, :dv], both[:, dv:].astype(BF), off, prod[:, dv:]


def local_rest(q, k, v, do, s0, rows, ib, p, gs):
    c = q.shape[0]
    row, col = indices(c)
    g_col, g_row, g_last, beta, cd, to_end = decays(rows)
    qn, rq = unit(q.astype(F32))
    kn, _ = unit(k.astype(F32))
    qb, kb, sb = qn.astype(BF), kn.astype(BF), s0.astype(BF)
    gamma = jnp.where(row == col, 1.0, gs)
    z = v.astype(F32) - cd * mm(kb, sb)
    ub = mm(ib, beta * z).astype(BF)
    prod = mm(do, jnp.concatenate([ub, sb], axis=0), 1, 1)
    dp, dos = prod[:, :c], cd * prod[:, c:]
    gdp = (gamma * dp).astype(BF)
    dq = unit_back(dos + mm(gdp, kb), qn, rq)
    dk0 = mm(gdp, qb, 0, 0)
    t = dp * p
    dg0 = jnp.sum((t + dos * qn).T, axis=0, keepdims=True) - jnp.sum(t, axis=0, keepdims=True)
    return dq, z, ub, dk0, dg0


def carry_head(k, v, s0, e, rows, ub, w0, nb, z, gram, gs, dk0, dg0):
    c = k.shape[0]
    g_col, g_row, g_last, beta, cd, to_end = decays(rows)
    kn, rk = unit(k.astype(F32))
    kb = kn.astype(BF)
    w = w0 + mm(nb, e)
    wb = w.astype(BF)
    dv = beta * w
    prod = mm(wb, jnp.concatenate([ub, s0.astype(BF)], axis=0), 1, 1)
    da, ws = -prod[:, :c], prod[:, c:]
    ue = to_end * mm(ub, e, 1, 1)
    dkk = (beta * gs * da).astype(BF)
    dkn = dk0 - (beta * cd) * ws + mm(dkk, kb) + mm(dkk, kb, 0, 0) + ue
    dk = unit_back(dkn, kn, rk)
    dagram = da * gram
    t = beta * dagram
    s = kn * ue
    dbeta = jnp.sum((dagram + w * z).T, axis=0, keepdims=True)
    dg = dg0 - jnp.sum(t, axis=0, keepdims=True)
    dg = dg + jnp.sum((t - dv * (v.astype(F32) - z) - s).T, axis=0, keepdims=True)
    tail = jnp.sum(s, keepdims=True) + jnp.exp(g_last) * jnp.sum(s0 * e.astype(F32), keepdims=True)
    lane = lax.broadcasted_iota(jnp.int32, (1, c), 1)
    dg = dg + jnp.where(lane == c - 1, tail, 0.0)
    return dv, dk, dg, dbeta


def split3(x):
    hi = x.astype(BF)
    rest = x - hi.astype(F32)
    mid = rest.astype(BF)
    return hi, mid, (rest - mid.astype(F32)).astype(BF)


def group_size(n, heads):
    size = 1
    while (2 * size) ** 2 <= n and heads % (2 * size) == 0 and n % (2 * size) == 0:
        size *= 2
    return size


def whole_kernel(
    n, m, size,
    q, k, v, do, s0, rows, fac, hidden, weights,
    dq, dk, dv, gh, gd, gw,
    pmat, gram, gs, invs, w0, nb, z, ub, dk0, dg0, dgs, dbs,
    maps, maps_in, tcomp, bcomp, gcomp, zin, zout, eout, ein,
    tbuf, got, part, gathered, ggot, wgot,
    map_sems, map_recv, z_sems, e_send, e_recv, sum_sems, head_sems,
):
    me, side = lax.axis_index("seq"), lax.axis_index("head")
    mesh_id = pl.DeviceIdType.MESH
    heads, c, dkk = q.shape
    dvv = v.shape[2]
    own = heads // size
    planes = n // size
    plane, rank = me // size, lax.rem(me, size)
    lag = planes - 1 - plane
    barrier = pltpu.get_barrier_semaphore()

    def run(low, high, body):
        def step(d, _):
            body(d)
            return 0

        lax.fori_loop(low, high, step, 0)

    def ahead(d):
        return lax.rem(me + d, n)

    def behind(d):
        return lax.rem(me + n - d, n)

    def side_ahead(d):
        return lax.rem(side + d, m)

    def side_behind(d):
        return lax.rem(side + m - d, m)

    def greet(d):
        pl.semaphore_signal(barrier, inc=1, device_id={"seq": ahead(d)}, device_id_type=mesh_id)

    def greet_side(d):
        pl.semaphore_signal(
            barrier, inc=1, device_id={"head": side_ahead(d)}, device_id_type=mesh_id
        )

    run(1, n, greet)
    run(1, m, greet_side)

    def send_map(b, to, source):
        return pltpu.make_async_remote_copy(
            src_ref=maps.at[b, to], dst_ref=maps_in.at[b, source],
            send_sem=map_sems.at[b, to], recv_sem=map_recv.at[b, source],
            device_id={"seq": plane * size + to}, device_id_type=mesh_id,
        )

    def send_plane(b):
        return pltpu.make_async_remote_copy(
            src_ref=zout.at[b], dst_ref=zin.at[b],
            send_sem=z_sems.at[0, b], recv_sem=z_sems.at[1, b],
            device_id={"seq": lax.rem(me + n - size, n)}, device_id_type=mesh_id,
        )

    def send_back(b, to, owner):
        return pltpu.make_async_remote_copy(
            src_ref=eout.at[b, to], dst_ref=ein.at[owner * own + b],
            send_sem=e_send.at[b, to], recv_sem=e_recv.at[owner * own + b],
            device_id={"seq": plane * size + to}, device_id_type=mesh_id,
        )

    def scatter(to, source):
        return pltpu.make_async_remote_copy(
            src_ref=tbuf.at[to], dst_ref=got.at[source],
            send_sem=sum_sems.at[0, to], recv_sem=sum_sems.at[1, source],
            device_id={"seq": to}, device_id_type=mesh_id,
        )

    def gather(to, source):
        return pltpu.make_async_remote_copy(
            src_ref=part, dst_ref=gathered.at[source],
            send_sem=sum_sems.at[2, to], recv_sem=sum_sems.at[3, source],
            device_id={"seq": to}, device_id_type=mesh_id,
        )

    def send_weights(to, source):
        return pltpu.make_async_remote_copy(
            src_ref=weights.at[to], dst_ref=wgot.at[source],
            send_sem=head_sems.at[0, to], recv_sem=head_sems.at[1, source],
            device_id={"head": to}, device_id_type=mesh_id,
        )

    def send_grads(to, source):
        return pltpu.make_async_remote_copy(
            src_ref=ggot.at[side], dst_ref=ggot.at[source],
            send_sem=head_sems.at[2, to], recv_sem=head_sems.at[3, source],
            device_id={"head": to}, device_id_type=mesh_id,
        )

    @pl.when(lag == 0)
    def _():
        zin[...] = jnp.zeros(zin.shape, BF)

    def local_batch(b):
        hs = [j * own + b for j in range(size)]
        firsts = [local_first(q[h], k[h], rows[h]) for h in hs]
        solved = inverses([first[5] for first in firsts])
        for j, h in enumerate(hs):
            first = firsts[j]
            ib, w0_, nb_, off, tt = local_map(do[h], solved[j], first)
            pmat[h], gram[h], gs[h] = first[2], first[3], first[4]
            invs[h], w0[h], nb[h] = ib, w0_, nb_
            last = jnp.broadcast_to(first[9], (8, dvv))
            high = last.astype(BF)
            low = (last - high.astype(F32)).astype(BF)
            message = jnp.concatenate([tt.astype(BF), off.astype(BF), high, low], axis=0)
            maps[b, j] = message

            @pl.when(rank == j)
            def _():
                maps_in[b, j] = message

    def local_sends(b):
        for j in range(size):

            @pl.when(rank != j)
            def _():
                send_map(b, j, rank).start()

    def piece(b, p):
        t = maps_in[b, p, :dkk]
        off = maps_in[b, p, dkk : 2 * dkk].astype(F32)
        ends = maps_in[b, p, 2 * dkk :].astype(F32)
        return t, off, ends[0:1] + ends[8:9]

    def compose(b):
        for p in range(size):

            @pl.when(rank != p)
            def _():
                send_map(b, p, p).wait_recv()

        t, bc, g = piece(b, size - 1)
        tc = t.astype(F32)
        for p in range(size - 2, -1, -1):
            t, off, last = piece(b, p)
            prod = mm(t, jnp.concatenate([tc.astype(BF), bc.astype(BF)], axis=1))
            tc = last * tc + g * t.astype(F32) - prod[:, :dkk]
            bc = last * bc + off - prod[:, dkk:]
            g = last * g
        tcomp[b] = tc.astype(BF)
        bcomp[b] = bc
        gcomp[b] = jnp.broadcast_to(g, gcomp.shape[1:])

    def hand_on(b):
        @pl.when(lag > 0)
        def _():
            send_plane(b).wait_recv()

        eb = zin[b]

        @pl.when(plane > 0)
        def _():
            e = gcomp[b, 0:1] * eb.astype(F32) + bcomp[b] - mm(tcomp[b], eb)
            zout[b] = e.astype(BF)
            send_plane(b).start()

        e = eb.astype(F32)
        for p in range(size - 1, -1, -1):
            eout[b, p] = eb

            @pl.when(rank == p)
            def _():
                ein[rank * own + b] = eb

            @pl.when(rank != p)
            def _():
                send_back(b, p, rank).start()

            if p > 0:
                t, off, last = piece(b, p)
                e = last * e + off - mm(t, eb)
                eb = e.astype(BF)

    def rest_batch(b):
        for j in range(size):
            h = j * own + b
            outs = local_rest(q[h], k[h], v[h], do[h], s0[h], rows[h], invs[h], pmat[h], gs[h])
            dq[h] = outs[0].astype(BF)
            z[h], ub[h], dk0[h], dg0[h] = outs[1:]

    def carry_batch(b):
        for j in range(size):

            @pl.when(rank != j)
            def _():
                send_back(b, rank, j).wait_recv()

        for j in range(size):
            h = j * own + b
            outs = carry_head(
                k[h], v[h], s0[h], ein[h], rows[h], ub[h], w0[h], nb[h], z[h], gram[h], gs[h],
                dk0[h], dg0[h],
            )
            dv[h] = outs[0].astype(BF)
            dk[h] = outs[1].astype(BF)
            dgs[pl.ds(h, 1), :] = outs[2]
            dbs[pl.ds(h, 1), :] = outs[3]

    late = max(own, planes) + 1

    def step(s):
        @pl.when(s < own)
        def _():
            local_batch(s)

            @pl.when(s == 0)
            def _():
                pl.semaphore_wait(barrier, n + m - 2)
                run(1, m, lambda d: send_weights(side_ahead(d), side).start())

            local_sends(s)

        turn = s - 1 - lag

        @pl.when((lag > 0) & (turn >= 0) & (turn < own))
        def _():
            hand_on(turn)

        @pl.when(s == own)
        def _():
            run(0, own, rest_batch)

        @pl.when((s >= 1) & (s <= own))
        def _():
            compose(s - 1)

            @pl.when(lag == 0)
            def _():
                hand_on(s - 1)

        @pl.when(s >= late)
        def _():
            carry_batch(s - late)

    run(0, own + late, step)

    row, col = indices(c)
    tri = jnp.where(row >= col, 1.0, 0.0).astype(BF)
    sums = mm(jnp.concatenate(split3(dgs[...]), axis=0), tri)
    dlog = sums[:heads] + sums[heads : 2 * heads] + sums[2 * heads :]
    grads = jnp.concatenate([dlog * fac[:heads], dbs[...] * fac[heads:]], axis=0).astype(BF)
    ggot[side] = grads
    run(1, m, lambda d: send_grads(side_ahead(d), side).start())
    width = hidden.shape[1]
    w = width // n
    terms = mm(grads, hidden[...])
    for i in range(n):
        tbuf[i] = terms[:, i * w : (i + 1) * w].astype(BF)
    run(1, n, lambda d: scatter(ahead(d), me).start())
    wgot[side] = weights[side]

    def partner(d):
        source = side_behind(d)
        send_weights(source, source).wait_recv()
        send_grads(source, source).wait_recv()

    run(1, m, partner)
    total = mm(ggot[0], wgot[0], 0, 0)
    for i in range(1, m):
        total = total + mm(ggot[i], wgot[i], 0, 0)
    gh[...] = total.astype(BF)

    def add(d, acc):
        source = behind(d)
        scatter(source, source).wait_recv()
        return acc + got[source].astype(F32)

    acc = lax.fori_loop(1, n, add, tbuf[me].astype(F32)).astype(BF)
    part[...] = acc
    gathered[me] = acc
    run(1, n, lambda d: gather(ahead(d), me).start())

    def arrive(d):
        source = behind(d)
        gather(source, source).wait_recv()

    run(1, n, arrive)
    for i in range(n):
        both = gathered[i].astype(F32)
        gd[:, i * w : (i + 1) * w] = both[:heads]
        gw[:, i * w : (i + 1) * w] = both[heads:]

    def done(b):
        for j in range(size):

            @pl.when(rank != j)
            def _():
                send_map(b, j, rank).wait_send()
                send_back(b, j, rank).wait_send()

        @pl.when(plane > 0)
        def _():
            send_plane(b).wait_send()

    run(0, own, done)
    run(1, n, lambda d: scatter(ahead(d), me).wait_send())
    run(1, n, lambda d: gather(ahead(d), me).wait_send())
    run(1, m, lambda d: send_weights(side_ahead(d), side).wait_send())
    run(1, m, lambda d: send_grads(side_ahead(d), side).wait_send())


def whole_part(n, m, q, k, v, do, s0, rows, fac, hidden, weights):
    h, c, dk = q.shape
    dv = v.shape[2]
    size = group_size(n, h)
    own = h // size
    width = hidden.shape[1]
    vm = pl.BlockSpec(memory_space=pltpu.VMEM)
    sd = jax.ShapeDtypeStruct
    dma = pltpu.SemaphoreType.DMA
    message = (2 * dk + 16, dv)
    return pl.pallas_call(
        partial(whole_kernel, n, m, size),
        out_shape=(
            sd((h, c, dk), BF), sd((h, c, dk), BF), sd((h, c, dv), BF), sd((c, width // m), BF),
            sd((h, width), F32), sd((h, width), F32),
        ),
        in_specs=[vm] * 9,
        out_specs=(vm,) * 6,
        scratch_shapes=[
            pltpu.VMEM((h, c, c), F32), pltpu.VMEM((h, c, c), F32), pltpu.VMEM((h, c, c), F32),
            pltpu.VMEM((h, c, c), BF), pltpu.VMEM((h, c, dv), F32), pltpu.VMEM((h, c, dk), BF),
            pltpu.VMEM((h, c, dv), F32), pltpu.VMEM((h, c, dv), BF), pltpu.VMEM((h, c, dk), F32),
            pltpu.VMEM((h, 1, c), F32), pltpu.VMEM((h, c), F32), pltpu.VMEM((h, c), F32),
            pltpu.VMEM((own, size) + message, BF), pltpu.VMEM((own, size) + message, BF),
            pltpu.VMEM((own, dk, dk), BF), pltpu.VMEM((own, dk, dv), F32),
            pltpu.VMEM((own, 8, dv), F32),
            pltpu.VMEM((own, dk, dv), BF), pltpu.VMEM((own, dk, dv), BF),
            pltpu.VMEM((own, size, dk, dv), BF), pltpu.VMEM((h, dk, dv), BF),
            pltpu.VMEM((n, 2 * h, width // n), BF), pltpu.VMEM((n, 2 * h, width // n), BF),
            pltpu.VMEM((2 * h, width // n), BF), pltpu.VMEM((n, 2 * h, width // n), BF),
            pltpu.VMEM((m, 2 * h, c), BF), pltpu.VMEM((m, 2 * h, width // m), BF),
            dma((own, size)), dma((own, size)), dma((2, own)), dma((own, size)), dma((h,)),
            dma((4, n)), dma((4, m)),
        ],
        compiler_params=pltpu.CompilerParams(
            collective_id=0, has_side_effects=True, vmem_limit_bytes=56 * 1024 * 1024
        ),
    )(q, k, v, do, s0, rows, fac, hidden, weights)


def gates(hidden_in, both, decay_bias, decay_log, write_bias):
    h = decay_bias.shape[0]
    logits = lax.dot_general(
        both, hidden_in, (((0,), (1,)), ((), ())), preferred_element_type=F32
    )
    pre = logits[:h] + decay_bias[:, None]
    rate = jnp.exp(decay_log)[:, None]
    beta = jax.nn.sigmoid(logits[h:] + write_bias[:, None])
    log_decay = -rate * jax.nn.softplus(pre)
    c = log_decay.shape[1]
    ones = jnp.triu(jnp.ones((c, c), F32))
    g = jnp.dot(log_decay, ones, precision=HI)
    return pre, rate, beta, g, ones


def shards(
    queries,
    key_vectors,
    values,
    out_grad,
    hidden_in,
    decay_weight,
    write_weight,
    decay_bias,
    decay_log,
    write_bias,
    start_state,
):
    n, m = lax.axis_size("seq"), lax.axis_size("head")
    both = jnp.concatenate([decay_weight, write_weight], axis=1)
    pre, rate, beta, g, _ = gates(hidden_in, both, decay_bias, decay_log, write_bias)
    h, c = g.shape
    rows = jnp.concatenate(
        [g[:, None], beta[:, None], jnp.zeros((h, 6, c), F32)], axis=1
    )
    fac = jnp.concatenate([-rate * jax.nn.sigmoid(pre), beta * (1.0 - beta)], axis=0)
    width = hidden_in.shape[1]
    weights = jnp.swapaxes(both.T.reshape(2 * h, m, width // m), 0, 1)
    q, k, v, do = (jnp.swapaxes(a, 0, 1) for a in (queries, key_vectors, values, out_grad))
    dq, dk, dv, gh, gd, gw = whole_part(
        n, m, q, k, v, do, start_state[0], rows, fac, hidden_in, weights
    )
    return (
        jnp.swapaxes(dq, 0, 1),
        jnp.swapaxes(dk, 0, 1),
        jnp.swapaxes(dv, 0, 1),
        gh,
        gd.T,
        gw.T,
    )


def solution(mesh):
    placed = (
        P("seq", "head", None),
        P("seq", "head", None),
        P("seq", "head", None),
        P("seq", "head", None),
        P("seq", None),
        P(None, "head"),
        P(None, "head"),
        P("head"),
        P("head"),
        P("head"),
        P("seq", "head", None, None),
    )
    return jax.shard_map(
        shards,
        mesh=mesh,
        in_specs=placed,
        out_specs=(
            P("seq", "head", None),
            P("seq", "head", None),
            P("seq", "head", None),
            P("seq", "head"),
            P(None, "head"),
            P(None, "head"),
        ),
        check_vma=False,
    )
```

```python
from functools import partial

import jax
import jax.numpy as jnp
from jax import lax
from jax.experimental import pallas as pl
from jax.experimental.pallas import tpu as pltpu
from jax.sharding import PartitionSpec as P

EPSILON = 1e-06
F32 = jnp.float32
BF = jnp.bfloat16


def mm(a, b, ca=1, cb=0):
    return lax.dot_general(
        a.astype(BF), b.astype(BF), (((ca,), (cb,)), ((), ())), preferred_element_type=F32
    )


def indices(c):
    row = lax.broadcasted_iota(jnp.int32, (c, c), 0)
    col = lax.broadcasted_iota(jnp.int32, (c, c), 1)
    return row, col


def inverses(couplings):
    c = couplings[0].shape[0]
    row, col = indices(c)
    invs = [
        jnp.where(row == col, 1.0, jnp.where((row ^ col) == 1, -a, 0.0)) for a in couplings
    ]
    level = 1
    while (2 << level) <= c:
        near = ((row >> level) ^ (col >> level)) == 1
        halves = [mm(x, jnp.where(near, a, 0.0)) for x, a in zip(invs, couplings)]
        invs = [x - mm(y, x) for x, y in zip(invs, halves)]
        level += 1
    return invs


def head_masks(c):
    row, col = indices(c)
    return row == col, col >= row, col > row


def down(x):
    return jnp.sum(x, axis=0, keepdims=True)


def to_col(eye, row):
    return jnp.sum(jnp.where(eye, row, 0.0), axis=1, keepdims=True)


def to_row(eye, x):
    return down(jnp.where(eye, jnp.sum(x, axis=1, keepdims=True), 0.0))


def scale_of(x):
    return lax.rsqrt(down(x * x) + EPSILON)


def local_first(q, k, rows):
    c = q.shape[0]
    eye, upper, strict = head_masks(c)
    g, beta = rows[0:1], rows[1:2]
    qt, kt = q.T, k.T
    rq, rk = scale_of(qt.astype(F32)), scale_of(kt.astype(F32))
    start = to_col(eye, jnp.log(rk) - g)
    decay = jnp.exp(jnp.where(upper, start + g, -1e30))
    grams = mm(k, jnp.concatenate([k, q], axis=0), 1, 1)
    kk = grams[:, :c]
    pt = decay * rq * grams[:, c:]
    pairs = jnp.where(strict, decay, 0.0) * rk
    return qt, kt, rq, rk, decay, pairs, kk, pt, beta * pairs * kk


def local_map(k, do, rows, inv, first):
    qt, kt, rq, rk, decay, pairs, kk, pt, a = first
    beta, cd, to_end = rows[1:2], rows[2:3], rows[3:4]
    dv = do.shape[1]
    ptdo = mm(pt, do).astype(BF)
    left = jnp.concatenate([inv.astype(BF), (inv * (to_end * rk)).astype(BF)], axis=1)
    right = jnp.concatenate(
        [
            jnp.concatenate([ptdo, jnp.zeros(k.shape, BF)], axis=1),
            jnp.concatenate([jnp.zeros(do.shape, BF), k], axis=1),
        ],
        axis=0,
    )
    both = mm(left, right)
    left = jnp.concatenate(
        [(qt * (cd * rq)).astype(BF), (kt * (-beta * cd * rk)).astype(BF)], axis=1
    )
    right = jnp.concatenate(
        [jnp.concatenate([do, jnp.zeros(k.shape, BF)], axis=1), both.astype(BF)], axis=0
    )
    return both[:, :dv], both[:, dv:], mm(left, right)


def local_rest(k, v, do, s0, rows, qt, kt, rq, rk, decay, pt, inv):
    c = k.shape[0]
    eye, _, _ = head_masks(c)
    beta, cd = rows[1:2], rows[2:3]
    sb = s0.astype(BF)
    ks = mm(k, sb)
    back = inv.T
    left = jnp.concatenate([back * beta, back * (-beta * cd * rk)], axis=1)
    ub = mm(left, jnp.concatenate([v, ks.astype(BF)], axis=0)).astype(BF)
    prod = mm(jnp.concatenate([ub, sb], axis=0), do, 1, 1)
    dpt, dost = prod[:c], prod[c:] * cd
    t = dpt * pt
    gdp = (decay * dpt).astype(BF)
    qn = qt * rq
    dqn = rq * (dost + mm(kt, gdp))
    dq = dqn - qn * down(qn * dqn)
    dk0 = mm(qn, gdp, 1, 1)
    dg0 = down(t) + down(dost * qn) - to_row(eye, t)
    return dq.astype(BF).T, ks, ub, dk0, dg0


def carry_head(v, s0, e, rows, kt, rk, pairs, kk, ub, w0, nb, ks, dk0, dg0):
    c = v.shape[0]
    eye, _, _ = head_masks(c)
    beta, cd, to_end = rows[1:2], rows[2:3], rows[3:4]
    w = w0 + mm(nb, e)
    wb = w.astype(BF)
    dv = to_col(eye, beta) * w
    prod = mm(jnp.concatenate([ub, s0.astype(BF)], axis=0), wb, 1, 1)
    da = -prod[:c] * pairs
    ue = (to_end * rk) * mm(e, ub, 1, 1)
    pair = (beta * da).astype(BF)
    kn = kt * rk
    dkn = dk0 - (beta * cd * rk) * prod[c:] + mm(kt, pair) + mm(kt, pair, 1, 1) + ue
    dk = dkn - kn * down(kn * dkn)
    da = da * kk
    own = down(da)
    wks = (cd * rk) * to_row(eye, w * ks)
    dbeta = own + to_row(eye, w * v.astype(F32)) - wks
    s = down(kt * ue)
    dg = dg0 + beta * (own - wks) - to_row(eye, beta * da) - s
    last = cd[:, c - 1 :]
    tail = jnp.sum(s, keepdims=True) + last * jnp.sum(down(s0 * e.astype(F32)), keepdims=True)
    lane = lax.broadcasted_iota(jnp.int32, (1, c), 1)
    dg = dg + jnp.where(lane == c - 1, tail, 0.0)
    return dv, dk.astype(BF).T, dg, dbeta


def split3(x):
    hi = x.astype(BF)
    rest = x - hi.astype(F32)
    mid = rest.astype(BF)
    return hi, mid, (rest - mid.astype(F32)).astype(BF)


def group_size(n, heads):
    size = 1
    while (2 * size) ** 2 <= n and heads % (2 * size) == 0 and n % (2 * size) == 0:
        size *= 2
    return size


def whole_kernel(
    n, m, size,
    q, k, v, do, s0, hidden, decay_w, write_w, decay_bias, decay_log, write_bias,
    dq, dk, dv, gh, gd, gw,
    rows, fac, weights, qts, kts, scales, decay, pairs, kks, pts, invs, w0, nb, ks, ub, dk0, dg0, dgs, dbs,
    maps, maps_in, tcomp, bcomp, gcomp, zin, zout, eout, ein,
    tbuf, got, part, gathered, ggot, wgot,
    map_sems, map_recv, z_sems, e_send, e_recv, sum_sems, head_sems,
):
    me, side = lax.axis_index("seq"), lax.axis_index("head")
    mesh_id = pl.DeviceIdType.MESH
    heads, c, dkk = q.shape
    dvv = v.shape[2]
    own = heads // size
    planes = n // size
    plane, rank = me // size, lax.rem(me, size)
    lag = planes - 1 - plane
    barrier = pltpu.get_barrier_semaphore()

    def run(low, high, body):
        def step(d, _):
            body(d)
            return 0

        lax.fori_loop(low, high, step, 0)

    def ahead(d):
        return lax.rem(me + d, n)

    def behind(d):
        return lax.rem(me + n - d, n)

    def side_ahead(d):
        return lax.rem(side + d, m)

    def side_behind(d):
        return lax.rem(side + m - d, m)

    def greet(d):
        pl.semaphore_signal(barrier, inc=1, device_id={"seq": ahead(d)}, device_id_type=mesh_id)

    def greet_side(d):
        pl.semaphore_signal(
            barrier, inc=1, device_id={"head": side_ahead(d)}, device_id_type=mesh_id
        )

    run(1, n, greet)
    run(1, m, greet_side)
    width = hidden.shape[1]
    w = width // n

    def send_map(b, to, source):
        return pltpu.make_async_remote_copy(
            src_ref=maps.at[b, to], dst_ref=maps_in.at[b, source],
            send_sem=map_sems.at[b, to], recv_sem=map_recv.at[b, source],
            device_id={"seq": plane * size + to}, device_id_type=mesh_id,
        )

    def send_plane(b):
        return pltpu.make_async_remote_copy(
            src_ref=zout.at[b], dst_ref=zin.at[b],
            send_sem=z_sems.at[0, b], recv_sem=z_sems.at[1, b],
            device_id={"seq": lax.rem(me + n - size, n)}, device_id_type=mesh_id,
        )

    def send_back(b, to, owner):
        return pltpu.make_async_remote_copy(
            src_ref=eout.at[b, to], dst_ref=ein.at[owner * own + b],
            send_sem=e_send.at[b, to], recv_sem=e_recv.at[owner * own + b],
            device_id={"seq": plane * size + to}, device_id_type=mesh_id,
        )

    def scatter(to, source):
        return pltpu.make_async_remote_copy(
            src_ref=tbuf.at[to], dst_ref=got.at[source],
            send_sem=sum_sems.at[0, to], recv_sem=sum_sems.at[1, source],
            device_id={"seq": to}, device_id_type=mesh_id,
        )

    def gather(to, source):
        return pltpu.make_async_remote_copy(
            src_ref=part, dst_ref=gathered.at[source],
            send_sem=sum_sems.at[2, to], recv_sem=sum_sems.at[3, source],
            device_id={"seq": to}, device_id_type=mesh_id,
        )

    def send_weights(to, source):
        return pltpu.make_async_remote_copy(
            src_ref=weights.at[to], dst_ref=wgot.at[source],
            send_sem=head_sems.at[0, to], recv_sem=head_sems.at[1, source],
            device_id={"head": to}, device_id_type=mesh_id,
        )

    def send_grads(to, source):
        return pltpu.make_async_remote_copy(
            src_ref=ggot.at[side], dst_ref=ggot.at[source],
            send_sem=head_sems.at[2, to], recv_sem=head_sems.at[3, source],
            device_id={"head": to}, device_id_type=mesh_id,
        )

    @pl.when(lag == 0)
    def _():
        zin[...] = jnp.zeros(zin.shape, BF)

    def prepare():
        eye = head_masks(heads)[0]
        for i in range(m):
            cut = pl.ds(i * (width // m), width // m)
            weights[i] = jnp.concatenate([decay_w[:, cut], write_w[:, cut]], axis=0)
        logits = mm(jnp.concatenate([decay_w[...], write_w[...]], axis=0), hidden[...], 1, 1)
        pre = logits[:heads] + to_col(eye, decay_bias[...])
        rate = jnp.exp(to_col(eye, decay_log[...]))
        beta = jax.nn.sigmoid(logits[heads:] + to_col(eye, write_bias[...]))
        log_decay = -rate * (jnp.maximum(pre, 0.0) + jnp.log1p(jnp.exp(-jnp.abs(pre))))
        row, col = indices(c)
        tri = jnp.where(row <= col, 1.0, 0.0).astype(BF)
        sums = mm(jnp.concatenate(split3(log_decay), axis=0), tri)
        g = sums[:heads] + sums[heads : 2 * heads] + sums[2 * heads :]
        fac[:heads] = -rate * jax.nn.sigmoid(pre)
        fac[heads:] = beta * (1.0 - beta)
        parts = (g, beta, jnp.exp(g), jnp.exp(g[:, c - 1 :] - g))
        for h in range(heads):
            for i, a in enumerate(parts):
                rows[h, i : i + 1] = a[h : h + 1]

    def wait_barrier():
        pl.semaphore_wait(barrier, n + m - 2)

    def local_batch(b):
        hs = [j * own + b for j in range(size)]
        firsts = [local_first(q[h], k[h], rows[h]) for h in hs]
        solved = inverses([first[8] for first in firsts])
        messages = []
        for j, h in enumerate(hs):
            qt, kt, rq, rk, decay_, pairs_, kk, pt, _ = firsts[j]
            w0_, nb_, made = local_map(k[h], do[h], rows[h], solved[j], firsts[j])
            qts[h], kts[h] = qt, kt
            scales[h, 0:1] = rq
            scales[h, 1:2] = rk
            decay[h], pairs[h], kks[h], pts[h] = decay_, pairs_, kk, pt
            invs[h], w0[h], nb[h] = solved[j].astype(BF), w0_, nb_.astype(BF)
            last = jnp.broadcast_to(rows[h][2:3, c - 1 :], (8, dvv + dkk))
            high = last.astype(BF)
            low = (last - high.astype(F32)).astype(BF)
            messages.append(jnp.concatenate([made.astype(BF), high, low], axis=0))
            maps[b, j] = messages[j]

        for j in range(size):

            @pl.when(rank == j)
            def _():
                maps_in[b, j] = messages[j]

    def local_sends(b):
        for j in range(size):

            @pl.when(rank != j)
            def _():
                send_map(b, j, rank).start()

    def piece(b, p):
        made = maps_in[b, p, :dkk]
        ends = maps_in[b, p, dkk:].astype(F32)
        return made, ends[0:1] + ends[8:9]

    def wait_maps(b):
        for p in range(size):

            @pl.when(rank != p)
            def _():
                send_map(b, p, p).wait_recv()

    def compose(b):
        wait_maps(b)
        made, g = piece(b, size - 1)
        both = made.astype(F32)
        for p in range(size - 2, -1, -1):
            made, last = piece(b, p)
            step = made.astype(F32)
            prod = mm(made[:, dvv:], both)
            both = last * both + jnp.concatenate(
                [step[:, :dvv], g[:, dvv:] * step[:, dvv:]], axis=1
            ) + prod
            g = last * g
        bcomp[b] = both[:, :dvv]
        tcomp[b] = both[:, dvv:].astype(BF)
        gcomp[b] = jnp.broadcast_to(g[:, :dvv], gcomp.shape[1:])

    def wait_plane(b):
        @pl.when(lag > 0)
        def _():
            send_plane(b).wait_recv()

    def hand_on(b):
        wait_plane(b)
        eb = zin[b]

        @pl.when(plane > 0)
        def _():
            e = gcomp[b, 0:1] * eb.astype(F32) + bcomp[b] + mm(tcomp[b], eb)
            zout[b] = e.astype(BF)
            send_plane(b).start()

        e = eb.astype(F32)
        for p in range(size - 1, -1, -1):
            eout[b, p] = eb

            @pl.when(rank == p)
            def _():
                ein[rank * own + b] = eb

            @pl.when(rank != p)
            def _():
                send_back(b, p, rank).start()

            if p > 0:
                made, last = piece(b, p)
                e = last[:, :dvv] * e + made[:, :dvv].astype(F32) + mm(made[:, dvv:], eb)
                eb = e.astype(BF)

    def rest_batch(b):
        for j in range(size):
            h = j * own + b
            dq[h], ks[h], ub[h], dk0[h], dg0[h] = local_rest(
                k[h], v[h], do[h], s0[h], rows[h], qts[h], kts[h],
                scales[h, 0:1], scales[h, 1:2], decay[h], pts[h], invs[h],
            )

    def wait_back(b):
        for j in range(size):

            @pl.when(rank != j)
            def _():
                send_back(b, rank, j).wait_recv()

    def carry_batch(b):
        wait_back(b)
        for j in range(size):
            h = j * own + b
            outs = carry_head(
                v[h], s0[h], ein[h], rows[h], kts[h], scales[h, 1:2], pairs[h], kks[h], ub[h],
                w0[h], nb[h], ks[h], dk0[h], dg0[h],
            )
            dv[h] = outs[0].astype(BF)
            dk[h] = outs[1]
            dgs[pl.ds(h, 1), :] = outs[2]
            dbs[pl.ds(h, 1), :] = outs[3]

    late = max(own, planes) + 1
    half = (own + 1) // 2

    def step(s):
        @pl.when(s < own)
        def _():
            local_batch(s)

            @pl.when(s == 0)
            def _():
                wait_barrier()
                run(1, m, lambda d: send_weights(side_ahead(d), side).start())

            local_sends(s)

        turn = s - 1 - lag

        @pl.when((lag > 0) & (turn >= 0) & (turn < own))
        def _():
            hand_on(turn)

        @pl.when(s == own)
        def _():
            run(0, half, rest_batch)

        @pl.when((s >= 1) & (s <= own))
        def _():
            compose(s - 1)

            @pl.when(lag == 0)
            def _():
                hand_on(s - 1)

        @pl.when((s > own) & (s < 2 * own + 1 - half))
        def _():
            rest_batch(s - own - 1 + half)

        @pl.when(s >= late)
        def _():
            carry_batch(s - late)

    prepare()
    run(0, own + late, step)

    def finish_grads():
        row, col = indices(c)
        tri = jnp.where(row >= col, 1.0, 0.0).astype(BF)
        sums = mm(jnp.concatenate(split3(dgs[...]), axis=0), tri)
        dlog = sums[:heads] + sums[heads : 2 * heads] + sums[2 * heads :]
        grads = jnp.concatenate([dlog * fac[:heads], dbs[...] * fac[heads:]], axis=0).astype(BF)
        ggot[side] = grads
        run(1, m, lambda d: send_grads(side_ahead(d), side).start())
        return grads

    def weight_terms(grads):
        terms = mm(grads, hidden[...])
        for i in range(n):
            tbuf[i] = terms[:, i * w : (i + 1) * w].astype(BF)
        run(1, n, lambda d: scatter(ahead(d), me).start())

    def partner(d):
        source = side_behind(d)
        send_weights(source, source).wait_recv()
        send_grads(source, source).wait_recv()

    def input_grad():
        wgot[side] = weights[side]
        run(1, m, partner)
        total = mm(ggot[0], wgot[0], 0, 0)
        for i in range(1, m):
            total = total + mm(ggot[i], wgot[i], 0, 0)
        gh[...] = total.astype(BF)

    def reduce_terms():
        def add(d, acc):
            source = behind(d)
            scatter(source, source).wait_recv()
            return acc + got[source].astype(F32)

        acc = lax.fori_loop(1, n, add, tbuf[me].astype(F32)).astype(BF)
        part[...] = acc
        gathered[me] = acc
        run(1, n, lambda d: gather(ahead(d), me).start())

    def arrive(d):
        source = behind(d)
        gather(source, source).wait_recv()

    def arrivals():
        run(1, n, arrive)

    def write_sums():
        for i in range(n):
            both = gathered[i].astype(F32)
            gd[:, i * w : (i + 1) * w] = both[:heads]
            gw[:, i * w : (i + 1) * w] = both[heads:]

    def done(b):
        for j in range(size):

            @pl.when(rank != j)
            def _():
                send_map(b, j, rank).wait_send()
                send_back(b, j, rank).wait_send()

        @pl.when(plane > 0)
        def _():
            send_plane(b).wait_send()

    weight_terms(finish_grads())
    input_grad()
    reduce_terms()
    arrivals()
    write_sums()
    run(0, own, done)
    run(1, n, lambda d: scatter(ahead(d), me).wait_send())
    run(1, n, lambda d: gather(ahead(d), me).wait_send())
    run(1, m, lambda d: send_weights(side_ahead(d), side).wait_send())
    run(1, m, lambda d: send_grads(side_ahead(d), side).wait_send())


def whole_part(n, m, q, k, v, do, s0, hidden, *gates):
    h, c, dk = q.shape
    dv = v.shape[2]
    size = group_size(n, h)
    own = h // size
    width = hidden.shape[1]
    vm = pl.BlockSpec(memory_space=pltpu.VMEM)
    sd = jax.ShapeDtypeStruct
    dma = pltpu.SemaphoreType.DMA
    message = (dk + 16, dv + dk)
    return pl.pallas_call(
        partial(whole_kernel, n, m, size),
        out_shape=(
            sd((h, c, dk), BF), sd((h, c, dk), BF), sd((h, c, dv), BF), sd((c, width // m), BF),
            sd((h, width), F32), sd((h, width), F32),
        ),
        in_specs=[vm] * 11,
        out_specs=(vm,) * 6,
        scratch_shapes=[
            pltpu.VMEM((h, 8, c), F32), pltpu.VMEM((2 * h, c), F32),
            pltpu.VMEM((m, 2 * h, width // m), BF),
            pltpu.VMEM((h, dk, c), BF), pltpu.VMEM((h, dk, c), BF), pltpu.VMEM((h, 8, c), F32),
            pltpu.VMEM((h, c, c), F32), pltpu.VMEM((h, c, c), F32), pltpu.VMEM((h, c, c), F32),
            pltpu.VMEM((h, c, c), F32), pltpu.VMEM((h, c, c), BF), pltpu.VMEM((h, c, dv), F32),
            pltpu.VMEM((h, c, dk), BF), pltpu.VMEM((h, c, dv), F32), pltpu.VMEM((h, c, dv), BF),
            pltpu.VMEM((h, dk, c), F32),
            pltpu.VMEM((h, 1, c), F32), pltpu.VMEM((h, c), F32), pltpu.VMEM((h, c), F32),
            pltpu.VMEM((own, size) + message, BF), pltpu.VMEM((own, size) + message, BF),
            pltpu.VMEM((own, dk, dk), BF), pltpu.VMEM((own, dk, dv), F32),
            pltpu.VMEM((own, 8, dv), F32),
            pltpu.VMEM((own, dk, dv), BF), pltpu.VMEM((own, dk, dv), BF),
            pltpu.VMEM((own, size, dk, dv), BF), pltpu.VMEM((h, dk, dv), BF),
            pltpu.VMEM((n, 2 * h, width // n), BF), pltpu.VMEM((n, 2 * h, width // n), BF),
            pltpu.VMEM((2 * h, width // n), BF), pltpu.VMEM((n, 2 * h, width // n), BF),
            pltpu.VMEM((m, 2 * h, c), BF), pltpu.VMEM((m, 2 * h, width // m), BF),
            dma((own, size)), dma((own, size)), dma((2, own)), dma((own, size)), dma((h,)),
            dma((4, n)), dma((4, m)),
        ],
        compiler_params=pltpu.CompilerParams(
            collective_id=0, has_side_effects=True, vmem_limit_bytes=28 * 1024 * 1024
        ),
    )(q, k, v, do, s0, hidden, *gates)


def shards(
    queries,
    key_vectors,
    values,
    out_grad,
    hidden_in,
    decay_weight,
    write_weight,
    decay_bias,
    decay_log,
    write_bias,
    start_state,
):
    n, m = lax.axis_size("seq"), lax.axis_size("head")
    q, k, v, do = (jnp.swapaxes(a, 0, 1) for a in (queries, key_vectors, values, out_grad))
    dq, dk, dv, gh, gd, gw = whole_part(
        n, m, q, k, v, do, start_state[0], hidden_in, decay_weight.T, write_weight.T,
        decay_bias[None], decay_log[None], write_bias[None],
    )
    return (
        jnp.swapaxes(dq, 0, 1),
        jnp.swapaxes(dk, 0, 1),
        jnp.swapaxes(dv, 0, 1),
        gh,
        gd.T,
        gw.T,
    )


def solution(mesh):
    placed = (
        P("seq", "head", None),
        P("seq", "head", None),
        P("seq", "head", None),
        P("seq", "head", None),
        P("seq", None),
        P(None, "head"),
        P(None, "head"),
        P("head"),
        P("head"),
        P("head"),
        P("seq", "head", None, None),
    )
    return jax.shard_map(
        shards,
        mesh=mesh,
        in_specs=placed,
        out_specs=(
            P("seq", "head", None),
            P("seq", "head", None),
            P("seq", "head", None),
            P("seq", "head"),
            P(None, "head"),
            P(None, "head"),
        ),
        check_vma=False,
    )
```

```python
from functools import partial

import jax
import jax.numpy as jnp
from jax import lax
from jax.experimental import pallas as pl
from jax.experimental.pallas import tpu as pltpu
from jax.sharding import PartitionSpec as P

EPSILON = 1e-06
F32 = jnp.float32
BF = jnp.bfloat16


def mm(a, b, ca=1, cb=0):
    return lax.dot_general(
        a.astype(BF), b.astype(BF), (((ca,), (cb,)), ((), ())), preferred_element_type=F32
    )


def indices(c):
    row = lax.broadcasted_iota(jnp.int32, (c, c), 0)
    col = lax.broadcasted_iota(jnp.int32, (c, c), 1)
    return row, col


def lockstep(*groups):
    results = [[None] * len(members) for members, _ in groups]
    active = {(i, j) for i, (members, _) in enumerate(groups) for j in range(len(members))}
    tick = 0
    while active:
        for i, (members, period) in enumerate(groups):
            for j, member in enumerate(members):
                if (i, j) in active and tick % period == 0:
                    try:
                        next(member)
                    except StopIteration as end:
                        results[i][j] = end.value
                        active.remove((i, j))
        tick += 1
    return results


def inverse(a):
    c = a.shape[0]
    row, col = indices(c)
    inv = jnp.where(row == col, 1.0, jnp.where((row ^ col) == 1, -a, 0.0))
    level = 1
    while (2 << level) <= c:
        near = ((row >> level) ^ (col >> level)) == 1
        half = mm(inv, jnp.where(near, a, 0.0))
        yield
        step = mm(half, inv)
        yield
        inv = inv - step
        level += 1
    return inv


def head_masks(c):
    row, col = indices(c)
    return row == col, col >= row, col > row


def down(x):
    return jnp.sum(x, axis=0, keepdims=True)


def to_col(eye, row):
    return jnp.sum(jnp.where(eye, row, 0.0), axis=1, keepdims=True)


def to_row(eye, x):
    return down(jnp.where(eye, jnp.sum(x, axis=1, keepdims=True), 0.0))


def scale_of(x):
    return lax.rsqrt(down(x * x) + EPSILON)


def local_head(q, k, do, rows):
    c = q.shape[0]
    dv = do.shape[1]
    eye, upper, strict = head_masks(c)
    g, beta, cd, to_end = rows[0:1], rows[1:2], rows[2:3], rows[3:4]
    qt, kt = q.T, k.T
    grams = mm(k, jnp.concatenate([k, q], axis=0), 1, 1)
    yield
    rq, rk = scale_of(qt.astype(F32)), scale_of(kt.astype(F32))
    start = to_col(eye, jnp.log(rk) - g)
    decay = jnp.exp(jnp.where(upper, start + g, -1e30))
    kk = grams[:, :c]
    pt = decay * rq * grams[:, c:]
    pairs = jnp.where(strict, decay, 0.0) * rk
    ptdo = mm(pt, do).astype(BF)
    inv = yield from inverse(beta * pairs * kk)
    left = jnp.concatenate([inv.astype(BF), (inv * (to_end * rk)).astype(BF)], axis=1)
    right = jnp.concatenate(
        [
            jnp.concatenate([ptdo, jnp.zeros(k.shape, BF)], axis=1),
            jnp.concatenate([jnp.zeros(do.shape, BF), k], axis=1),
        ],
        axis=0,
    )
    both = mm(left, right)
    yield
    left = jnp.concatenate(
        [(qt * (cd * rq)).astype(BF), (kt * (-beta * cd * rk)).astype(BF)], axis=1
    )
    right = jnp.concatenate(
        [jnp.concatenate([do, jnp.zeros(k.shape, BF)], axis=1), both.astype(BF)], axis=0
    )
    made = mm(left, right)
    yield
    return qt, kt, rq, rk, decay, pairs, kk, pt, inv, both[:, :dv], both[:, dv:], made


def local_rest(k, v, do, s0, rows, qt, kt, rq, rk, decay, pt, inv):
    c = k.shape[0]
    eye, _, _ = head_masks(c)
    beta, cd = rows[1:2], rows[2:3]
    sb = s0.astype(BF)
    ks = mm(k, sb)
    back = inv.T
    yield
    left = jnp.concatenate([back * beta, back * (-beta * cd * rk)], axis=1)
    ub = mm(left, jnp.concatenate([v, ks.astype(BF)], axis=0)).astype(BF)
    yield
    prod = mm(jnp.concatenate([ub, sb], axis=0), do, 1, 1)
    yield
    dpt, dost = prod[:c], prod[c:] * cd
    t = dpt * pt
    gdp = (decay * dpt).astype(BF)
    qn = qt * rq
    dqk = mm(kt, gdp)
    dk0 = mm(qn, gdp, 1, 1)
    yield
    dg0 = down(t) + down(dost * qn) - to_row(eye, t)
    dqn = rq * (dost + dqk)
    dq = dqn - qn * down(qn * dqn)
    yield
    return dq.astype(BF).T, ks, ub, dk0, dg0


def carry_head(v, s0, e, rows, kt, rk, pairs, kk, ub, w0, nb, ks, dk0, dg0):
    c = v.shape[0]
    eye, _, _ = head_masks(c)
    beta, cd, to_end = rows[1:2], rows[2:3], rows[3:4]
    w = w0 + mm(nb, e)
    ue = mm(e, ub, 1, 1)
    yield
    wb = w.astype(BF)
    prod = mm(jnp.concatenate([ub, s0.astype(BF)], axis=0), wb, 1, 1)
    ue = (to_end * rk) * ue
    s = down(kt * ue)
    wv = to_row(eye, w * v.astype(F32))
    wks = (cd * rk) * to_row(eye, w * ks)
    yield
    da = -prod[:c] * pairs
    pair = (beta * da).astype(BF)
    kn = kt * rk
    dkn = dk0 - (beta * cd * rk) * prod[c:] + ue
    near, far = mm(kt, pair), mm(kt, pair, 1, 1)
    da = da * kk
    own = down(da)
    dbeta = own + wv - wks
    dg = dg0 + beta * (own - wks) - to_row(eye, beta * da) - s
    yield
    dkn = dkn + near + far
    dk = dkn - kn * down(kn * dkn)
    last = cd[:, c - 1 :]
    tail = jnp.sum(s, keepdims=True) + last * jnp.sum(down(s0 * e.astype(F32)), keepdims=True)
    lane = lax.broadcasted_iota(jnp.int32, (1, c), 1)
    dg = dg + jnp.where(lane == c - 1, tail, 0.0)
    dv = to_col(eye, beta) * w
    yield
    return dv, dk.astype(BF).T, dg, dbeta


def split3(x):
    hi = x.astype(BF)
    rest = x - hi.astype(F32)
    mid = rest.astype(BF)
    return hi, mid, (rest - mid.astype(F32)).astype(BF)


def group_size(n, heads):
    size = 1
    while (2 * size) ** 2 <= n and heads % (2 * size) == 0 and n % (2 * size) == 0:
        size *= 2
    return size


def whole_kernel(
    n, m, size,
    q, k, v, do, s0, hidden, decay_w, write_w, decay_bias, decay_log, write_bias,
    dq_out, dk_out, dv_out, gh, gd, gw,
    dq, dk, dv, rows, fac, weights, qts, kts, scales, decay, pairs, kks, pts, invs, w0, nb, ks, ub, dk0, dg0, dgs, dbs,
    ends, ends_in, maps, maps_in, tcomp, bcomp, gcomp, zin, zout, eout, ein,
    tbuf, got, part, gathered, ggot, wgot,
    end_sems, map_sems, map_recv, z_sems, e_send, e_recv, sum_sems, head_sems,
):
    me, side = lax.axis_index("seq"), lax.axis_index("head")
    mesh_id = pl.DeviceIdType.MESH
    heads, c, dkk = q.shape
    dvv = v.shape[2]
    own = heads // size
    planes = n // size
    plane, rank = me // size, lax.rem(me, size)
    lag = planes - 1 - plane
    barrier = pltpu.get_barrier_semaphore()

    def run(low, high, body):
        def step(d, _):
            body(d)
            return 0

        lax.fori_loop(low, high, step, 0)

    def ahead(d):
        return lax.rem(me + d, n)

    def behind(d):
        return lax.rem(me + n - d, n)

    def side_ahead(d):
        return lax.rem(side + d, m)

    def side_behind(d):
        return lax.rem(side + m - d, m)

    def far_first(d):
        skip = jnp.where(plane < planes // 2, planes - 1 - d // size, d // size)
        return skip * size + lax.rem(rank + 1 + d, size)

    def to_all(start):
        def one(d):
            to = far_first(d)

            @pl.when(to != me)
            def _():
                start(to)

        run(0, n, one)

    def greet(d):
        pl.semaphore_signal(barrier, inc=1, device_id={"seq": ahead(d)}, device_id_type=mesh_id)

    def greet_side(d):
        pl.semaphore_signal(
            barrier, inc=1, device_id={"head": side_ahead(d)}, device_id_type=mesh_id
        )

    run(1, n, greet)
    run(1, m, greet_side)
    width = hidden.shape[1]
    w = width // n

    def send_map(b, to, source):
        return pltpu.make_async_remote_copy(
            src_ref=maps.at[b, to], dst_ref=maps_in.at[b, source],
            send_sem=map_sems.at[b, to], recv_sem=map_recv.at[b, source],
            device_id={"seq": plane * size + to}, device_id_type=mesh_id,
        )

    def send_ends(to, source):
        return pltpu.make_async_remote_copy(
            src_ref=ends, dst_ref=ends_in.at[source],
            send_sem=end_sems.at[0, to], recv_sem=end_sems.at[1, source],
            device_id={"seq": plane * size + to}, device_id_type=mesh_id,
        )

    def send_plane(b):
        return pltpu.make_async_remote_copy(
            src_ref=zout.at[b], dst_ref=zin.at[b],
            send_sem=z_sems.at[0, b], recv_sem=z_sems.at[1, b],
            device_id={"seq": lax.rem(me + n - size, n)}, device_id_type=mesh_id,
        )

    def send_back(b, to, owner):
        return pltpu.make_async_remote_copy(
            src_ref=eout.at[b, to], dst_ref=ein.at[owner * own + b],
            send_sem=e_send.at[b, to], recv_sem=e_recv.at[owner * own + b],
            device_id={"seq": plane * size + to}, device_id_type=mesh_id,
        )

    def scatter(to, source):
        return pltpu.make_async_remote_copy(
            src_ref=tbuf.at[to], dst_ref=got.at[source],
            send_sem=sum_sems.at[0, to], recv_sem=sum_sems.at[1, source],
            device_id={"seq": to}, device_id_type=mesh_id,
        )

    def gather(to, source):
        return pltpu.make_async_remote_copy(
            src_ref=part, dst_ref=gathered.at[source],
            send_sem=sum_sems.at[2, to], recv_sem=sum_sems.at[3, source],
            device_id={"seq": to}, device_id_type=mesh_id,
        )

    def send_weights(to, source):
        return pltpu.make_async_remote_copy(
            src_ref=weights.at[to], dst_ref=wgot.at[source],
            send_sem=head_sems.at[0, to], recv_sem=head_sems.at[1, source],
            device_id={"head": to}, device_id_type=mesh_id,
        )

    def send_grads(to, source):
        return pltpu.make_async_remote_copy(
            src_ref=ggot.at[side], dst_ref=ggot.at[source],
            send_sem=head_sems.at[2, to], recv_sem=head_sems.at[3, source],
            device_id={"head": to}, device_id_type=mesh_id,
        )

    @pl.when(lag == 0)
    def _():
        zin[...] = jnp.zeros(zin.shape, BF)

    def prepare():
        eye = head_masks(heads)[0]
        for i in range(m):
            cut = pl.ds(i * (width // m), width // m)
            weights[i] = jnp.concatenate([decay_w[:, cut], write_w[:, cut]], axis=0)
        logits = mm(jnp.concatenate([decay_w[...], write_w[...]], axis=0), hidden[...], 1, 1)
        pre = logits[:heads] + to_col(eye, decay_bias[...])
        rate = jnp.exp(to_col(eye, decay_log[...]))
        beta = jax.nn.sigmoid(logits[heads:] + to_col(eye, write_bias[...]))
        log_decay = -rate * (jnp.maximum(pre, 0.0) + jnp.log1p(jnp.exp(-jnp.abs(pre))))
        row, col = indices(c)
        tri = jnp.where(row <= col, 1.0, 0.0).astype(BF)
        sums = mm(jnp.concatenate(split3(log_decay), axis=0), tri)
        g = sums[:heads] + sums[heads : 2 * heads] + sums[2 * heads :]
        fac[:heads] = -rate * jax.nn.sigmoid(pre)
        fac[heads:] = beta * (1.0 - beta)
        parts = (g, beta, jnp.exp(g), jnp.exp(g[:, c - 1 :] - g))
        ends[...] = jnp.broadcast_to(parts[2][:, c - 1 :], ends.shape)
        ends_in[rank] = jnp.broadcast_to(parts[2][:, c - 1 :], ends.shape)
        for h in range(heads):
            for i, a in enumerate(parts):
                rows[h, i : i + 1] = a[h : h + 1]

    def wait_barrier():
        pl.semaphore_wait(barrier, n + m - 2)

    def batch_heads(b):
        return [j * own + b for j in range(size)]

    def local_parts(b):
        return [local_head(q[h], k[h], do[h], rows[h]) for h in batch_heads(b)]

    def local_store(b, outs):
        for j, h in enumerate(batch_heads(b)):
            qts[h], kts[h], rq, rk, decay[h], pairs[h], kks[h], pts[h], inv, w0_, nb_, made = outs[j]
            scales[h, 0:1] = rq
            scales[h, 1:2] = rk
            invs[h], w0[h], nb[h] = inv.astype(BF), w0_, nb_.astype(BF)
            maps[b, j] = made.astype(BF)

    def rest_parts(b):
        return [
            local_rest(
                k[h], v[h], do[h], s0[h], rows[h], qts[h], kts[h],
                scales[h, 0:1], scales[h, 1:2], decay[h], pts[h], invs[h],
            )
            for h in batch_heads(b)
        ]

    def rest_store(b, outs):
        for j, h in enumerate(batch_heads(b)):
            dq[h], ks[h], ub[h], dk0[h], dg0[h] = outs[j]

    def local_batch(b):
        local_store(b, lockstep((local_parts(b), 1))[0])

    def rest_batch(b):
        rest_store(b, lockstep((rest_parts(b), 1))[0])

    def both_batches(s):
        outs = lockstep((rest_parts(s - 1), 2), (local_parts(s), 1))
        rest_store(s - 1, outs[0])
        local_store(s, outs[1])

    def end_sends():
        for j in range(size):

            @pl.when(rank != j)
            def _():
                send_ends(j, rank).start()

    def wait_ends():
        for p in range(size):

            @pl.when(rank != p)
            def _():
                send_ends(p, p).wait_recv()

    def local_sends(b):
        for j in range(size):

            @pl.when(rank != j)
            def _():
                send_map(b, j, rank).start()

        maps_in[b, rank] = maps[b, rank]

    def piece(b, p):
        return maps_in[b, p], ends_in[p, pl.ds(rank * own + b, 1), :]

    def wait_maps(b):
        for p in range(size):

            @pl.when(rank != p)
            def _():
                send_map(b, p, p).wait_recv()

    def compose(b):
        wait_maps(b)
        made, g = piece(b, size - 1)
        both = made.astype(F32)
        for p in range(size - 2, -1, -1):
            made, last = piece(b, p)
            step = made.astype(F32)
            prod = mm(made[:, dvv:], both)
            both = last[:, :1] * both + jnp.concatenate(
                [step[:, :dvv], g[:, :1] * step[:, dvv:]], axis=1
            ) + prod
            g = last * g
        bcomp[b] = both[:, :dvv]
        tcomp[b] = both[:, dvv:].astype(BF)
        gcomp[b] = jnp.broadcast_to(g, gcomp.shape[1:])

    def wait_plane(b):
        @pl.when(lag > 0)
        def _():
            send_plane(b).wait_recv()

    def hand_on(b):
        wait_plane(b)
        eb = zin[b]

        @pl.when(plane > 0)
        def _():
            e = gcomp[b, 0:1] * eb.astype(F32) + bcomp[b] + mm(tcomp[b], eb)
            zout[b] = e.astype(BF)
            send_plane(b).start()

    def hand_back(b):
        eb = zin[b]
        e = eb.astype(F32)
        for p in range(size - 1, -1, -1):
            eout[b, p] = eb

            @pl.when(rank == p)
            def _():
                ein[rank * own + b] = eb

            @pl.when(rank != p)
            def _():
                send_back(b, p, rank).start()

            if p > 0:
                made, last = piece(b, p)
                e = last * e + made[:, :dvv].astype(F32) + mm(made[:, dvv:], eb)
                eb = e.astype(BF)

    def wait_back(b):
        for j in range(size):

            @pl.when(rank != j)
            def _():
                send_back(b, rank, j).wait_recv()

    def carry_batch(b):
        wait_back(b)
        parts = [
            carry_head(
                v[h], s0[h], ein[h], rows[h], kts[h], scales[h, 1:2], pairs[h], kks[h], ub[h],
                w0[h], nb[h], ks[h], dk0[h], dg0[h],
            )
            for h in batch_heads(b)
        ]
        outs = lockstep((parts, 1))[0]
        for j, h in enumerate(batch_heads(b)):
            dv[h] = outs[j][0].astype(BF)
            dk[h] = outs[j][1]
            dgs[pl.ds(h, 1), :] = outs[j][2]
            dbs[pl.ds(h, 1), :] = outs[j][3]

    late = max(own, planes) + 1

    def first_batch():
        local_batch(0)
        wait_barrier()
        run(1, m, lambda d: send_weights(side_ahead(d), side).start())
        end_sends()
        local_sends(0)

    def pass_on(s):
        turn = s - 1 - lag

        @pl.when((lag > 0) & (turn >= 0) & (turn < own))
        def _():
            hand_on(turn)

    def gather_maps(s):
        @pl.when(s == 1)
        def _():
            wait_ends()

        compose(s - 1)

        @pl.when(lag == 0)
        def _():
            hand_on(s - 1)

    def early(s):
        both_batches(s)
        local_sends(s)
        pass_on(s)
        gather_maps(s)

    def middle():
        pass_on(own)
        rest_batch(own - 1)
        gather_maps(own)
        run(0, jnp.maximum(own - lag, 0), hand_back)

    def later(s):
        pass_on(s)
        turn = s - 1 - lag

        @pl.when((turn >= 0) & (turn < own))
        def _():
            hand_back(turn)

        @pl.when(s >= late)
        def _():
            carry_batch(s - late)

    prepare()
    first_batch()
    run(1, own, early)
    middle()
    run(own + 1, own + late, later)

    def finish_grads():
        row, col = indices(c)
        tri = jnp.where(row >= col, 1.0, 0.0).astype(BF)
        sums = mm(jnp.concatenate(split3(dgs[...]), axis=0), tri)
        dlog = sums[:heads] + sums[heads : 2 * heads] + sums[2 * heads :]
        grads = jnp.concatenate([dlog * fac[:heads], dbs[...] * fac[heads:]], axis=0).astype(BF)
        ggot[side] = grads
        run(1, m, lambda d: send_grads(side_ahead(d), side).start())
        return grads

    def weight_terms(grads):
        terms = mm(grads, hidden[...])
        for i in range(n):
            tbuf[i] = terms[:, i * w : (i + 1) * w].astype(BF)
        to_all(lambda to: scatter(to, me).start())

    def partner(d):
        source = side_behind(d)
        send_weights(source, source).wait_recv()
        send_grads(source, source).wait_recv()

    def input_grad():
        wgot[side] = weights[side]
        run(1, m, partner)
        total = mm(ggot[0], wgot[0], 0, 0)
        for i in range(1, m):
            total = total + mm(ggot[i], wgot[i], 0, 0)
        gh[...] = total.astype(BF)

    def reduce_terms():
        def add(d, acc):
            source = behind(d)
            scatter(source, source).wait_recv()
            return acc + got[source].astype(F32)

        acc = lax.fori_loop(1, n, add, tbuf[me].astype(F32)).astype(BF)
        part[...] = acc
        gathered[me] = acc
        to_all(lambda to: gather(to, me).start())

    def arrive(d):
        source = behind(d)
        gather(source, source).wait_recv()

    def arrivals():
        run(1, n, arrive)

    def reorder():
        for ref, source in ((dq_out, dq), (dk_out, dk), (dv_out, dv)):
            ref[...] = jnp.swapaxes(source[...], 0, 1)

    def write_sums():
        for i in range(n):
            both = gathered[i].astype(F32)
            gd[:, i * w : (i + 1) * w] = both[:heads]
            gw[:, i * w : (i + 1) * w] = both[heads:]

    def done(b):
        for j in range(size):

            @pl.when(rank != j)
            def _():
                send_map(b, j, rank).wait_send()
                send_back(b, j, rank).wait_send()

        @pl.when(plane > 0)
        def _():
            send_plane(b).wait_send()

    weight_terms(finish_grads())
    input_grad()
    reduce_terms()
    reorder()
    arrivals()
    write_sums()
    for j in range(size):

        @pl.when(rank != j)
        def _():
            send_ends(j, rank).wait_send()

    run(0, own, done)
    run(1, n, lambda d: scatter(ahead(d), me).wait_send())
    run(1, n, lambda d: gather(ahead(d), me).wait_send())
    run(1, m, lambda d: send_weights(side_ahead(d), side).wait_send())
    run(1, m, lambda d: send_grads(side_ahead(d), side).wait_send())


def whole_part(n, m, q, k, v, do, s0, hidden, *gates):
    h, c, dk = q.shape
    dv = v.shape[2]
    size = group_size(n, h)
    own = h // size
    width = hidden.shape[1]
    vm = pl.BlockSpec(memory_space=pltpu.VMEM)
    sd = jax.ShapeDtypeStruct
    dma = pltpu.SemaphoreType.DMA
    message = (dk, dv + dk)
    return pl.pallas_call(
        partial(whole_kernel, n, m, size),
        out_shape=(
            sd((c, h, dk), BF), sd((c, h, dk), BF), sd((c, h, dv), BF), sd((c, width // m), BF),
            sd((h, width), F32), sd((h, width), F32),
        ),
        in_specs=[vm] * 11,
        out_specs=(vm,) * 6,
        scratch_shapes=[
            pltpu.VMEM((h, c, dk), BF), pltpu.VMEM((h, c, dk), BF), pltpu.VMEM((h, c, dv), BF),
            pltpu.VMEM((h, 8, c), F32), pltpu.VMEM((2 * h, c), F32),
            pltpu.VMEM((m, 2 * h, width // m), BF),
            pltpu.VMEM((h, dk, c), BF), pltpu.VMEM((h, dk, c), BF), pltpu.VMEM((h, 8, c), F32),
            pltpu.VMEM((h, c, c), F32), pltpu.VMEM((h, c, c), F32), pltpu.VMEM((h, c, c), F32),
            pltpu.VMEM((h, c, c), F32), pltpu.VMEM((h, c, c), BF), pltpu.VMEM((h, c, dv), F32),
            pltpu.VMEM((h, c, dk), BF), pltpu.VMEM((h, c, dv), F32), pltpu.VMEM((h, c, dv), BF),
            pltpu.VMEM((h, dk, c), F32),
            pltpu.VMEM((h, 1, c), F32), pltpu.VMEM((h, c), F32), pltpu.VMEM((h, c), F32),
            pltpu.VMEM((h, dv), F32), pltpu.VMEM((size, h, dv), F32),
            pltpu.VMEM((own, size) + message, BF), pltpu.VMEM((own, size) + message, BF),
            pltpu.VMEM((own, dk, dk), BF), pltpu.VMEM((own, dk, dv), F32),
            pltpu.VMEM((own, 8, dv), F32),
            pltpu.VMEM((own, dk, dv), BF), pltpu.VMEM((own, dk, dv), BF),
            pltpu.VMEM((own, size, dk, dv), BF), pltpu.VMEM((h, dk, dv), BF),
            pltpu.VMEM((n, 2 * h, width // n), BF), pltpu.VMEM((n, 2 * h, width // n), BF),
            pltpu.VMEM((2 * h, width // n), BF), pltpu.VMEM((n, 2 * h, width // n), BF),
            pltpu.VMEM((m, 2 * h, c), BF), pltpu.VMEM((m, 2 * h, width // m), BF),
            dma((2, size)), dma((own, size)), dma((own, size)), dma((2, own)), dma((own, size)), dma((h,)),
            dma((4, n)), dma((4, m)),
        ],
        compiler_params=pltpu.CompilerParams(
            collective_id=0, has_side_effects=True, vmem_limit_bytes=28 * 1024 * 1024
        ),
    )(q, k, v, do, s0, hidden, *gates)


def store_kernel(*refs):
    count = (len(refs) - 1) // 2
    sems = refs[-1]
    copies = [
        pltpu.make_async_copy(refs[i], refs[count + i], sems.at[i]) for i in range(count)
    ]
    for copy in copies:
        copy.start()
    for copy in copies:
        copy.wait()


def store_part(arrays):
    count = len(arrays)
    return pl.pallas_call(
        store_kernel,
        out_shape=tuple(jax.ShapeDtypeStruct(a.shape, a.dtype) for a in arrays),
        in_specs=[pl.BlockSpec(memory_space=pltpu.VMEM)] * count,
        out_specs=(pl.BlockSpec(memory_space=pl.ANY),) * count,
        scratch_shapes=[pltpu.SemaphoreType.DMA((count,))],
        compiler_params=pltpu.CompilerParams(vmem_limit_bytes=8 * 1024 * 1024),
    )(*arrays)


def shards(
    queries,
    key_vectors,
    values,
    out_grad,
    hidden_in,
    decay_weight,
    write_weight,
    decay_bias,
    decay_log,
    write_bias,
    start_state,
):
    n, m = lax.axis_size("seq"), lax.axis_size("head")
    q, k, v, do = (jnp.swapaxes(a, 0, 1) for a in (queries, key_vectors, values, out_grad))
    made = whole_part(
        n, m, q, k, v, do, start_state[0], hidden_in, decay_weight.T, write_weight.T,
        decay_bias[None], decay_log[None], write_bias[None],
    )
    dq, dk, dv, gh, gd, gw = store_part(made)
    return dq, dk, dv, gh, gd.T, gw.T


def solution(mesh):
    placed = (
        P("seq", "head", None),
        P("seq", "head", None),
        P("seq", "head", None),
        P("seq", "head", None),
        P("seq", None),
        P(None, "head"),
        P(None, "head"),
        P("head"),
        P("head"),
        P("head"),
        P("seq", "head", None, None),
    )
    return jax.shard_map(
        shards,
        mesh=mesh,
        in_specs=placed,
        out_specs=(
            P("seq", "head", None),
            P("seq", "head", None),
            P("seq", "head", None),
            P("seq", "head"),
            P(None, "head"),
            P(None, "head"),
        ),
        check_vma=False,
    )
```

```python
from functools import partial

import jax
import jax.numpy as jnp
from jax import lax
from jax.experimental import pallas as pl
from jax.experimental.pallas import tpu as pltpu
from jax.sharding import PartitionSpec as P

EPSILON = 1e-06
F32 = jnp.float32
BF = jnp.bfloat16


def mm(a, b, ca=1, cb=0):
    return lax.dot_general(
        a.astype(BF), b.astype(BF), (((ca,), (cb,)), ((), ())), preferred_element_type=F32
    )


def indices(c):
    row = lax.broadcasted_iota(jnp.int32, (c, c), 0)
    col = lax.broadcasted_iota(jnp.int32, (c, c), 1)
    return row, col


def lockstep(*groups):
    results = [[None] * len(members) for members, _ in groups]
    active = {(i, j) for i, (members, _) in enumerate(groups) for j in range(len(members))}
    tick = 0
    while active:
        for i, (members, period) in enumerate(groups):
            for j, member in enumerate(members):
                if (i, j) in active and tick % period == 0:
                    try:
                        next(member)
                    except StopIteration as end:
                        results[i][j] = end.value
                        active.remove((i, j))
        tick += 1
    return results


def inverse(a):
    c = a.shape[0]
    row, col = indices(c)
    inv = jnp.where(row == col, 1.0, jnp.where((row ^ col) == 1, -a, 0.0))
    level = 1
    while (2 << level) <= c:
        near = ((row >> level) ^ (col >> level)) == 1
        half = mm(inv, jnp.where(near, a, 0.0))
        yield
        step = mm(half, inv)
        yield
        inv = inv - step
        level += 1
    return inv


def head_masks(c):
    row, col = indices(c)
    return row == col, col >= row, col > row


def down(x):
    return jnp.sum(x, axis=0, keepdims=True)


def to_col(eye, row):
    return jnp.sum(jnp.where(eye, row, 0.0), axis=1, keepdims=True)


def to_row(eye, x):
    return down(jnp.where(eye, jnp.sum(x, axis=1, keepdims=True), 0.0))


def scale_of(x):
    return lax.rsqrt(down(x * x) + EPSILON)


def local_head(q, k, do, rows):
    c = q.shape[0]
    dv = do.shape[1]
    eye, upper, strict = head_masks(c)
    g, beta, cd, to_end = rows[0:1], rows[1:2], rows[2:3], rows[3:4]
    qt, kt = q.T, k.T
    grams = mm(k, jnp.concatenate([k, q], axis=0), 1, 1)
    yield
    rq, rk = scale_of(qt.astype(F32)), scale_of(kt.astype(F32))
    start = to_col(eye, jnp.log(rk) - g)
    decay = jnp.exp(jnp.where(upper, start + g, -1e30))
    kk = grams[:, :c]
    pt = decay * rq * grams[:, c:]
    pairs = jnp.where(strict, decay, 0.0) * rk
    ptdo = mm(pt, do).astype(BF)
    inv = yield from inverse(beta * pairs * kk)
    left = jnp.concatenate([inv.astype(BF), (inv * (to_end * rk)).astype(BF)], axis=1)
    right = jnp.concatenate(
        [
            jnp.concatenate([ptdo, jnp.zeros(k.shape, BF)], axis=1),
            jnp.concatenate([jnp.zeros(do.shape, BF), k], axis=1),
        ],
        axis=0,
    )
    both = mm(left, right)
    yield
    left = jnp.concatenate(
        [(qt * (cd * rq)).astype(BF), (kt * (-beta * cd * rk)).astype(BF)], axis=1
    )
    right = jnp.concatenate(
        [jnp.concatenate([do, jnp.zeros(k.shape, BF)], axis=1), both.astype(BF)], axis=0
    )
    made = mm(left, right)
    yield
    return qt, kt, rq, rk, decay, pairs, kk, pt, inv, both[:, :dv], both[:, dv:], made


def local_rest(k, v, do, s0, rows, qt, kt, rq, rk, decay, pt, inv):
    c = k.shape[0]
    eye, _, _ = head_masks(c)
    beta, cd = rows[1:2], rows[2:3]
    sb = s0.astype(BF)
    ks = mm(k, sb)
    back = inv.T
    yield
    left = jnp.concatenate([back * beta, back * (-beta * cd * rk)], axis=1)
    ub = mm(left, jnp.concatenate([v, ks.astype(BF)], axis=0)).astype(BF)
    yield
    prod = mm(jnp.concatenate([ub, sb], axis=0), do, 1, 1)
    yield
    dpt, dost = prod[:c], prod[c:] * cd
    t = dpt * pt
    gdp = (decay * dpt).astype(BF)
    qn = qt * rq
    dqk = mm(kt, gdp)
    dk0 = mm(qn, gdp, 1, 1)
    yield
    dg0 = down(t) + down(dost * qn) - to_row(eye, t)
    dqn = rq * (dost + dqk)
    dq = dqn - qn * down(qn * dqn)
    yield
    return dq.astype(BF).T, ks, ub, dk0, dg0


def carry_head(v, s0, e, rows, kt, rk, pairs, kk, ub, w0, nb, ks, dk0, dg0):
    c = v.shape[0]
    eye, _, _ = head_masks(c)
    beta, cd, to_end = rows[1:2], rows[2:3], rows[3:4]
    w = w0 + mm(nb, e)
    ue = mm(e, ub, 1, 1)
    yield
    wb = w.astype(BF)
    prod = mm(jnp.concatenate([ub, s0.astype(BF)], axis=0), wb, 1, 1)
    ue = (to_end * rk) * ue
    s = down(kt * ue)
    wv = to_row(eye, w * v.astype(F32))
    wks = (cd * rk) * to_row(eye, w * ks)
    yield
    da = -prod[:c] * pairs
    pair = (beta * da).astype(BF)
    kn = kt * rk
    dkn = dk0 - (beta * cd * rk) * prod[c:] + ue
    near, far = mm(kt, pair), mm(kt, pair, 1, 1)
    da = da * kk
    own = down(da)
    dbeta = own + wv - wks
    dg = dg0 + beta * (own - wks) - to_row(eye, beta * da) - s
    yield
    dkn = dkn + near + far
    dk = dkn - kn * down(kn * dkn)
    last = cd[:, c - 1 :]
    tail = jnp.sum(s, keepdims=True) + last * jnp.sum(down(s0 * e.astype(F32)), keepdims=True)
    lane = lax.broadcasted_iota(jnp.int32, (1, c), 1)
    dg = dg + jnp.where(lane == c - 1, tail, 0.0)
    dv = to_col(eye, beta) * w
    yield
    return dv, dk.astype(BF).T, dg, dbeta


def split3(x):
    hi = x.astype(BF)
    rest = x - hi.astype(F32)
    mid = rest.astype(BF)
    return hi, mid, (rest - mid.astype(F32)).astype(BF)


def group_size(n, heads):
    size = 1
    while (2 * size) ** 2 <= n and heads % (2 * size) == 0 and n % (2 * size) == 0:
        size *= 2
    return size


def whole_kernel(
    n, m, size,
    q_in, k_in, v_in, do_in, s0_in, hidden_in, decay_w_in, write_w_in,
    decay_bias_in, decay_log_in, write_bias_in,
    dq_out, dk_out, dv_out, gh, gd, gw,
    q_raw, k_raw, v_raw, do_raw, s0, hidden, decay_w, write_w, decay_bias, decay_log, write_bias,
    q, k, v, do, dq, dk, dv, rows, fac, weights, qts, kts, scales, decay, pairs, kks, pts, invs, w0, nb, ks, ub, dk0, dg0, dgs, dbs,
    ends, ends_in, maps, maps_in, tcomp, bcomp, gcomp, far_out, far_in, zin, zout, eout, ein,
    tbuf, got, part, gathered, ggot, wgot,
    in_sems, far_sems, end_sems, map_sems, map_recv, z_sems, e_send, e_recv, sum_sems, head_sems,
):
    me, side = lax.axis_index("seq"), lax.axis_index("head")
    mesh_id = pl.DeviceIdType.MESH
    heads, c, dkk = q.shape
    dvv = v.shape[2]
    own = heads // size
    planes = n // size
    plane, rank = me // size, lax.rem(me, size)
    lag = planes - 1 - plane
    direct = min(own, 2)
    chained = own - direct
    barrier = pltpu.get_barrier_semaphore()

    def run(low, high, body):
        def step(d, _):
            body(d)
            return 0

        lax.fori_loop(low, high, step, 0)

    def ahead(d):
        return lax.rem(me + d, n)

    def behind(d):
        return lax.rem(me + n - d, n)

    def side_ahead(d):
        return lax.rem(side + d, m)

    def side_behind(d):
        return lax.rem(side + m - d, m)

    def far_first(d):
        skip = jnp.where(plane < planes // 2, planes - 1 - d // size, d // size)
        return skip * size + lax.rem(rank + 1 + d, size)

    def to_all(start):
        def one(d):
            to = far_first(d)

            @pl.when(to != me)
            def _():
                start(to)

        run(0, n, one)

    def greet(d):
        pl.semaphore_signal(barrier, inc=1, device_id={"seq": ahead(d)}, device_id_type=mesh_id)

    def greet_side(d):
        pl.semaphore_signal(
            barrier, inc=1, device_id={"head": side_ahead(d)}, device_id_type=mesh_id
        )

    arrays = (
        (hidden_in, hidden), (decay_w_in, decay_w), (write_w_in, write_w),
        (decay_bias_in, decay_bias), (decay_log_in, decay_log), (write_bias_in, write_bias),
        (k_in, k_raw), (q_in, q_raw), (do_in, do_raw), (v_in, v_raw), (s0_in, s0),
    )
    loads = [pltpu.make_async_copy(a, b, in_sems.at[i]) for i, (a, b) in enumerate(arrays)]
    for load in loads:
        load.start()

    run(1, n, greet)
    run(1, m, greet_side)
    width = hidden.shape[1]
    w = width // n

    def send_map(b, to, source):
        return pltpu.make_async_remote_copy(
            src_ref=maps.at[b, to], dst_ref=maps_in.at[b, source],
            send_sem=map_sems.at[b, to], recv_sem=map_recv.at[b, source],
            device_id={"seq": plane * size + to}, device_id_type=mesh_id,
        )

    def send_ends(to, source):
        return pltpu.make_async_remote_copy(
            src_ref=ends, dst_ref=ends_in.at[source],
            send_sem=end_sems.at[0, to], recv_sem=end_sems.at[1, source],
            device_id={"seq": plane * size + to}, device_id_type=mesh_id,
        )

    def send_plane(b):
        return pltpu.make_async_remote_copy(
            src_ref=zout.at[b], dst_ref=zin.at[b],
            send_sem=z_sems.at[0, b], recv_sem=z_sems.at[1, b],
            device_id={"seq": lax.rem(me + n - size, n)}, device_id_type=mesh_id,
        )

    def send_far(i, to, source, part):
        return pltpu.make_async_remote_copy(
            src_ref=far_out.at[(i,) + part], dst_ref=far_in.at[(i, source) + part],
            send_sem=far_sems.at[0, i, to], recv_sem=far_sems.at[1, i, source],
            device_id={"seq": to * size + rank}, device_id_type=mesh_id,
        )

    whole_map = (pl.ds(0, dkk + 16), pl.ds(0, dvv + dkk))
    offset_only = (pl.ds(0, dkk), pl.ds(0, dvv))

    def send_back(b, to, owner):
        return pltpu.make_async_remote_copy(
            src_ref=eout.at[b, to], dst_ref=ein.at[owner * own + b],
            send_sem=e_send.at[b, to], recv_sem=e_recv.at[owner * own + b],
            device_id={"seq": plane * size + to}, device_id_type=mesh_id,
        )

    def scatter(to, source):
        return pltpu.make_async_remote_copy(
            src_ref=tbuf.at[to], dst_ref=got.at[source],
            send_sem=sum_sems.at[0, to], recv_sem=sum_sems.at[1, source],
            device_id={"seq": to}, device_id_type=mesh_id,
        )

    def gather(to, source):
        return pltpu.make_async_remote_copy(
            src_ref=part, dst_ref=gathered.at[source],
            send_sem=sum_sems.at[2, to], recv_sem=sum_sems.at[3, source],
            device_id={"seq": to}, device_id_type=mesh_id,
        )

    def send_weights(to, source):
        return pltpu.make_async_remote_copy(
            src_ref=weights.at[to], dst_ref=wgot.at[source],
            send_sem=head_sems.at[0, to], recv_sem=head_sems.at[1, source],
            device_id={"head": to}, device_id_type=mesh_id,
        )

    def send_grads(to, source):
        return pltpu.make_async_remote_copy(
            src_ref=ggot.at[side], dst_ref=ggot.at[source],
            send_sem=head_sems.at[2, to], recv_sem=head_sems.at[3, source],
            device_id={"head": to}, device_id_type=mesh_id,
        )

    @pl.when(lag == 0)
    def _():
        zin[...] = jnp.zeros(zin.shape, BF)

    def prepare():
        eye = head_masks(heads)[0]
        for i in range(m):
            cut = pl.ds(i * (width // m), width // m)
            weights[i] = jnp.concatenate([decay_w[:, cut], write_w[:, cut]], axis=0)
        logits = mm(jnp.concatenate([decay_w[...], write_w[...]], axis=0), hidden[...], 1, 1)
        pre = logits[:heads] + to_col(eye, decay_bias[...])
        rate = jnp.exp(to_col(eye, decay_log[...]))
        beta = jax.nn.sigmoid(logits[heads:] + to_col(eye, write_bias[...]))
        log_decay = -rate * (jnp.maximum(pre, 0.0) + jnp.log1p(jnp.exp(-jnp.abs(pre))))
        row, col = indices(c)
        tri = jnp.where(row <= col, 1.0, 0.0).astype(BF)
        sums = mm(jnp.concatenate(split3(log_decay), axis=0), tri)
        g = sums[:heads] + sums[heads : 2 * heads] + sums[2 * heads :]
        fac[:heads] = -rate * jax.nn.sigmoid(pre)
        fac[heads:] = beta * (1.0 - beta)
        parts = (g, beta, jnp.exp(g), jnp.exp(g[:, c - 1 :] - g))
        ends[...] = jnp.broadcast_to(parts[2][:, c - 1 :], ends.shape)
        ends_in[rank] = jnp.broadcast_to(parts[2][:, c - 1 :], ends.shape)
        for h in range(heads):
            for i, a in enumerate(parts):
                rows[h, i : i + 1] = a[h : h + 1]

    def wait_barrier():
        pl.semaphore_wait(barrier, n + m - 2)

    def batch_heads(b):
        return [j * own + b for j in range(size)]

    def local_parts(b):
        return [local_head(q[h], k[h], do[h], rows[h]) for h in batch_heads(b)]

    def local_store(b, outs):
        for j, h in enumerate(batch_heads(b)):
            qts[h], kts[h], rq, rk, decay[h], pairs[h], kks[h], pts[h], inv, w0_, nb_, made = outs[j]
            scales[h, 0:1] = rq
            scales[h, 1:2] = rk
            invs[h], w0[h], nb[h] = inv.astype(BF), w0_, nb_.astype(BF)
            maps[b, j] = made.astype(BF)

    def rest_parts(b):
        return [
            local_rest(
                k[h], v[h], do[h], s0[h], rows[h], qts[h], kts[h],
                scales[h, 0:1], scales[h, 1:2], decay[h], pts[h], invs[h],
            )
            for h in batch_heads(b)
        ]

    def rest_store(b, outs):
        for j, h in enumerate(batch_heads(b)):
            dq[h], ks[h], ub[h], dk0[h], dg0[h] = outs[j]

    def local_batch(b):
        local_store(b, lockstep((local_parts(b), 1))[0])

    def rest_batch(b):
        rest_store(b, lockstep((rest_parts(b), 1))[0])

    def both_batches(s):
        outs = lockstep((rest_parts(s - 1), 2), (local_parts(s), 1))
        rest_store(s - 1, outs[0])
        local_store(s, outs[1])

    def end_sends():
        for j in range(size):

            @pl.when(rank != j)
            def _():
                send_ends(j, rank).start()

    def wait_ends():
        for p in range(size):

            @pl.when(rank != p)
            def _():
                send_ends(p, p).wait_recv()

    def local_sends(b):
        for j in range(size):

            @pl.when(rank != j)
            def _():
                send_map(b, j, rank).start()

        maps_in[b, rank] = maps[b, rank]

    def piece(b, p):
        return maps_in[b, p], ends_in[p, pl.ds(rank * own + b, 1), :]

    def wait_maps(b):
        for p in range(size):

            @pl.when(rank != p)
            def _():
                send_map(b, p, p).wait_recv()

    def compose(b):
        wait_maps(b)
        made, g = piece(b, size - 1)
        both = made.astype(F32)
        for p in range(size - 2, -1, -1):
            made, last = piece(b, p)
            step = made.astype(F32)
            prod = mm(made[:, dvv:], both)
            both = last[:, :1] * both + jnp.concatenate(
                [step[:, :dvv], g[:, :1] * step[:, dvv:]], axis=1
            ) + prod
            g = last * g
        bcomp[b] = both[:, :dvv]
        tcomp[b] = both[:, dvv:].astype(BF)
        gcomp[b] = jnp.broadcast_to(g, gcomp.shape[1:])

    def wait_plane(b):
        @pl.when(lag > 0)
        def _():
            send_plane(b).wait_recv()

    def hand_on(b):
        wait_plane(b)
        eb = zin[b]

        @pl.when(plane > 0)
        def _():
            e = gcomp[b, 0:1] * eb.astype(F32) + bcomp[b] + mm(tcomp[b], eb)
            zout[b] = e.astype(BF)
            send_plane(b).start()

    def send_fars(b):
        i = b - chained
        g = gcomp[b]
        high = g.astype(BF)
        low = (g - high.astype(F32)).astype(BF)
        far_out[i, :dkk] = jnp.concatenate([bcomp[b].astype(BF), tcomp[b]], axis=1)
        far_out[i, dkk : dkk + 8, :dvv] = high
        far_out[i, dkk + 8 :, :dvv] = low

        @pl.when(lag == 0)
        def _():
            run(0, plane, lambda p: send_far(i, p, plane, offset_only).start())

        @pl.when(lag > 0)
        def _():
            run(0, plane, lambda p: send_far(i, p, plane, whole_map).start())

    def resolve(b):
        i = b - chained
        send_far(i, planes - 1, planes - 1, offset_only).wait_recv()

        def fold(d, e):
            source = planes - 2 - d
            send_far(i, source, source, whole_map).wait_recv()
            made = far_in[i, source, :dkk]
            g = far_in[i, source, dkk:, :dvv].astype(F32)
            prod = mm(made[:, dvv:], e)
            return (g[0:1] + g[8:9]) * e + made[:, :dvv].astype(F32) + prod

        e = far_in[i, planes - 1, :dkk, :dvv].astype(F32)
        zin[b] = lax.fori_loop(0, lag - 1, fold, e).astype(BF)

    def hand_back(b):
        eb = zin[b]
        e = eb.astype(F32)
        for p in range(size - 1, -1, -1):
            eout[b, p] = eb

            @pl.when(rank == p)
            def _():
                ein[rank * own + b] = eb

            @pl.when(rank != p)
            def _():
                send_back(b, p, rank).start()

            if p > 0:
                made, last = piece(b, p)
                e = last * e + made[:, :dvv].astype(F32) + mm(made[:, dvv:], eb)
                eb = e.astype(BF)

    def wait_back(b):
        for j in range(size):

            @pl.when(rank != j)
            def _():
                send_back(b, rank, j).wait_recv()

    def carry_batch(b):
        wait_back(b)
        parts = [
            carry_head(
                v[h], s0[h], ein[h], rows[h], kts[h], scales[h, 1:2], pairs[h], kks[h], ub[h],
                w0[h], nb[h], ks[h], dk0[h], dg0[h],
            )
            for h in batch_heads(b)
        ]
        outs = lockstep((parts, 1))[0]
        for j, h in enumerate(batch_heads(b)):
            dv[h] = outs[j][0].astype(BF)
            dk[h] = outs[j][1]
            dgs[pl.ds(h, 1), :] = outs[j][2]
            dbs[pl.ds(h, 1), :] = outs[j][3]

    late = max(own, planes) + 1


    def first_batch():
        local_batch(0)
        wait_barrier()
        run(1, m, lambda d: send_weights(side_ahead(d), side).start())
        end_sends()
        local_sends(0)

    def pass_on(s):
        turn = s - 1 - lag

        @pl.when((lag > 0) & (turn >= 0) & (turn < chained))
        def _():
            hand_on(turn)

        @pl.when((lag > 0) & (turn >= chained) & (turn < own))
        def _():
            resolve(turn)

    def gather_maps(s):
        @pl.when(s == 1)
        def _():
            wait_ends()

        compose(s - 1)

        @pl.when((lag == 0) & (s <= chained))
        def _():
            hand_on(s - 1)

        @pl.when((plane > 0) & (s > chained))
        def _():
            send_fars(s - 1)

    def early(s):
        both_batches(s)
        local_sends(s)
        pass_on(s)
        gather_maps(s)

    def middle():
        pass_on(own)
        rest_batch(own - 1)
        gather_maps(own)
        run(0, jnp.maximum(own - lag, 0), hand_back)

    def later(s):
        pass_on(s)
        turn = s - 1 - lag

        @pl.when((turn >= 0) & (turn < own))
        def _():
            hand_back(turn)

        @pl.when(s >= late)
        def _():
            carry_batch(s - late)

    def take(first, last, pairs):
        for load in loads[first:last]:
            load.wait()
        for ref, raw in pairs:
            ref[...] = jnp.swapaxes(raw[...], 0, 1)

    take(0, 6, ())
    prepare()
    take(6, 9, ((k, k_raw), (q, q_raw), (do, do_raw)))
    first_batch()
    take(9, 11, ((v, v_raw),))
    run(1, own, early)
    middle()
    run(own + 1, own + late, later)

    def finish_grads():
        row, col = indices(c)
        tri = jnp.where(row >= col, 1.0, 0.0).astype(BF)
        sums = mm(jnp.concatenate(split3(dgs[...]), axis=0), tri)
        dlog = sums[:heads] + sums[heads : 2 * heads] + sums[2 * heads :]
        grads = jnp.concatenate([dlog * fac[:heads], dbs[...] * fac[heads:]], axis=0).astype(BF)
        ggot[side] = grads
        run(1, m, lambda d: send_grads(side_ahead(d), side).start())
        return grads

    def weight_terms(grads):
        terms = mm(grads, hidden[...])
        for i in range(n):
            tbuf[i] = terms[:, i * w : (i + 1) * w].astype(BF)
        to_all(lambda to: scatter(to, me).start())

    def partner(d):
        source = side_behind(d)
        send_weights(source, source).wait_recv()
        send_grads(source, source).wait_recv()

    def input_grad():
        wgot[side] = weights[side]
        run(1, m, partner)
        total = mm(ggot[0], wgot[0], 0, 0)
        for i in range(1, m):
            total = total + mm(ggot[i], wgot[i], 0, 0)
        gh[...] = total.astype(BF)

    def reduce_terms():
        def add(d, acc):
            source = behind(d)
            scatter(source, source).wait_recv()
            return acc + got[source].astype(F32)

        acc = lax.fori_loop(1, n, add, tbuf[me].astype(F32)).astype(BF)
        part[...] = acc
        gathered[me] = acc
        to_all(lambda to: gather(to, me).start())

    def arrive(d):
        source = behind(d)
        gather(source, source).wait_recv()

    def arrivals():
        run(1, n, arrive)

    def reorder():
        for ref, source in ((dq_out, dq), (dk_out, dk), (dv_out, dv)):
            ref[...] = jnp.swapaxes(source[...], 0, 1)

    def write_sums():
        for i in range(n):
            both = gathered[i].astype(F32)
            gd[:, i * w : (i + 1) * w] = both[:heads]
            gw[:, i * w : (i + 1) * w] = both[heads:]

    def done(b):
        for j in range(size):

            @pl.when(rank != j)
            def _():
                send_map(b, j, rank).wait_send()
                send_back(b, j, rank).wait_send()

        @pl.when((plane > 0) & (b < chained))
        def _():
            send_plane(b).wait_send()

        @pl.when((b >= chained) & (lag == 0))
        def _():
            run(0, plane, lambda p: send_far(b - chained, p, plane, offset_only).wait_send())

        @pl.when((b >= chained) & (lag > 0))
        def _():
            run(0, plane, lambda p: send_far(b - chained, p, plane, whole_map).wait_send())

    weight_terms(finish_grads())
    input_grad()
    reduce_terms()
    reorder()
    arrivals()
    write_sums()
    for j in range(size):

        @pl.when(rank != j)
        def _():
            send_ends(j, rank).wait_send()

    run(0, own, done)
    run(1, n, lambda d: scatter(ahead(d), me).wait_send())
    run(1, n, lambda d: gather(ahead(d), me).wait_send())
    run(1, m, lambda d: send_weights(side_ahead(d), side).wait_send())
    run(1, m, lambda d: send_grads(side_ahead(d), side).wait_send())


def whole_part(n, m, q, k, v, do, s0, hidden, *gates):
    c, h, dk = q.shape
    dv = v.shape[2]
    size = group_size(n, h)
    own = h // size
    width = hidden.shape[1]
    vm = pl.BlockSpec(memory_space=pltpu.VMEM)
    sd = jax.ShapeDtypeStruct
    dma = pltpu.SemaphoreType.DMA
    message = (dk, dv + dk)
    return pl.pallas_call(
        partial(whole_kernel, n, m, size),
        out_shape=(
            pltpu.VMEM((c, h, dk), BF), pltpu.VMEM((c, h, dk), BF), pltpu.VMEM((c, h, dv), BF), pltpu.VMEM((c, width // m), BF),
            pltpu.VMEM((h, width), F32), pltpu.VMEM((h, width), F32),
        ),
        in_specs=[pl.BlockSpec(memory_space=pl.ANY)] * 11,
        out_specs=(vm,) * 6,
        scratch_shapes=[pltpu.VMEM(a.shape, a.dtype) for a in (q, k, v, do, s0, hidden) + gates]
        + [
            pltpu.VMEM((h, c, dk), BF), pltpu.VMEM((h, c, dk), BF), pltpu.VMEM((h, c, dv), BF),
            pltpu.VMEM((h, c, dv), BF),
            pltpu.VMEM((h, c, dk), BF), pltpu.VMEM((h, c, dk), BF), pltpu.VMEM((h, c, dv), BF),
            pltpu.VMEM((h, 8, c), F32), pltpu.VMEM((2 * h, c), F32),
            pltpu.VMEM((m, 2 * h, width // m), BF),
            pltpu.VMEM((h, dk, c), BF), pltpu.VMEM((h, dk, c), BF), pltpu.VMEM((h, 8, c), F32),
            pltpu.VMEM((h, c, c), F32), pltpu.VMEM((h, c, c), F32), pltpu.VMEM((h, c, c), F32),
            pltpu.VMEM((h, c, c), F32), pltpu.VMEM((h, c, c), BF), pltpu.VMEM((h, c, dv), F32),
            pltpu.VMEM((h, c, dk), BF), pltpu.VMEM((h, c, dv), F32), pltpu.VMEM((h, c, dv), BF),
            pltpu.VMEM((h, dk, c), F32),
            pltpu.VMEM((h, 1, c), F32), pltpu.VMEM((h, c), F32), pltpu.VMEM((h, c), F32),
            pltpu.VMEM((h, dv), F32), pltpu.VMEM((size, h, dv), F32),
            pltpu.VMEM((own, size) + message, BF), pltpu.VMEM((own, size) + message, BF),
            pltpu.VMEM((own, dk, dk), BF), pltpu.VMEM((own, dk, dv), F32),
            pltpu.VMEM((own, 8, dv), F32),
            pltpu.VMEM((min(own, 2), dk + 16, dv + dk), BF),
            pltpu.VMEM((min(own, 2), n // size, dk + 16, dv + dk), BF),
            pltpu.VMEM((own, dk, dv), BF), pltpu.VMEM((own, dk, dv), BF),
            pltpu.VMEM((own, size, dk, dv), BF), pltpu.VMEM((h, dk, dv), BF),
            pltpu.VMEM((n, 2 * h, width // n), BF), pltpu.VMEM((n, 2 * h, width // n), BF),
            pltpu.VMEM((2 * h, width // n), BF), pltpu.VMEM((n, 2 * h, width // n), BF),
            pltpu.VMEM((m, 2 * h, c), BF), pltpu.VMEM((m, 2 * h, width // m), BF),
            dma((11,)), dma((2, min(own, 2), n // size)), dma((2, size)), dma((own, size)), dma((own, size)), dma((2, own)), dma((own, size)), dma((h,)),
            dma((4, n)), dma((4, m)),
        ],
        compiler_params=pltpu.CompilerParams(
            collective_id=0, has_side_effects=True, vmem_limit_bytes=57000 * 1024
        ),
    )(q, k, v, do, s0, hidden, *gates)


def store_kernel(*refs):
    count = (len(refs) - 1) // 2
    sems = refs[-1]
    copies = [
        pltpu.make_async_copy(refs[i], refs[count + i], sems.at[i]) for i in range(count)
    ]
    for copy in copies:
        copy.start()
    for copy in copies:
        copy.wait()


def store_part(arrays):
    count = len(arrays)
    return pl.pallas_call(
        store_kernel,
        out_shape=tuple(jax.ShapeDtypeStruct(a.shape, a.dtype) for a in arrays),
        in_specs=[pl.BlockSpec(memory_space=pltpu.VMEM)] * count,
        out_specs=(pl.BlockSpec(memory_space=pl.ANY),) * count,
        scratch_shapes=[pltpu.SemaphoreType.DMA((count,))],
        compiler_params=pltpu.CompilerParams(vmem_limit_bytes=8 * 1024 * 1024),
    )(*arrays)


def shards(
    queries,
    key_vectors,
    values,
    out_grad,
    hidden_in,
    decay_weight,
    write_weight,
    decay_bias,
    decay_log,
    write_bias,
    start_state,
):
    n, m = lax.axis_size("seq"), lax.axis_size("head")
    made = whole_part(
        n, m, queries, key_vectors, values, out_grad, start_state[0], hidden_in, decay_weight.T, write_weight.T,
        decay_bias[None], decay_log[None], write_bias[None],
    )
    dq, dk, dv, gh, gd, gw = store_part(made)
    return dq, dk, dv, gh, gd.T, gw.T


def solution(mesh):
    placed = (
        P("seq", "head", None),
        P("seq", "head", None),
        P("seq", "head", None),
        P("seq", "head", None),
        P("seq", None),
        P(None, "head"),
        P(None, "head"),
        P("head"),
        P("head"),
        P("head"),
        P("seq", "head", None, None),
    )
    return jax.shard_map(
        shards,
        mesh=mesh,
        in_specs=placed,
        out_specs=(
            P("seq", "head", None),
            P("seq", "head", None),
            P("seq", "head", None),
            P("seq", "head"),
            P(None, "head"),
            P(None, "head"),
        ),
        check_vma=False,
    )
```

```python
from functools import partial

import jax
import jax.numpy as jnp
from jax import lax
from jax.experimental import pallas as pl
from jax.experimental.pallas import tpu as pltpu
from jax.sharding import PartitionSpec as P

EPSILON = 1e-06
F32 = jnp.float32
BF = jnp.bfloat16


def mm(a, b, ca=1, cb=0):
    return lax.dot_general(
        a.astype(BF), b.astype(BF), (((ca,), (cb,)), ((), ())), preferred_element_type=F32
    )


def indices(c):
    row = lax.broadcasted_iota(jnp.int32, (c, c), 0)
    col = lax.broadcasted_iota(jnp.int32, (c, c), 1)
    return row, col


def lockstep(*groups):
    results = [[None] * len(members) for members, _ in groups]
    active = {(i, j) for i, (members, _) in enumerate(groups) for j in range(len(members))}
    tick = 0
    while active:
        for i, (members, period) in enumerate(groups):
            for j, member in enumerate(members):
                if (i, j) in active and tick % period == 0:
                    try:
                        next(member)
                    except StopIteration as end:
                        results[i][j] = end.value
                        active.remove((i, j))
        tick += 1
    return results


def inverse(a):
    c = a.shape[0]
    row, col = indices(c)
    inv = jnp.where(row == col, 1.0, jnp.where((row ^ col) == 1, -a, 0.0))
    level = 1
    while (2 << level) <= c:
        near = ((row >> level) ^ (col >> level)) == 1
        half = mm(inv, jnp.where(near, a, 0.0))
        yield
        step = mm(half, inv)
        yield
        inv = inv - step
        level += 1
    return inv


def head_masks(c):
    row, col = indices(c)
    return row == col, col >= row, col > row


def down(x):
    return jnp.sum(x, axis=0, keepdims=True)


def to_col(eye, row):
    return jnp.sum(jnp.where(eye, row, 0.0), axis=1, keepdims=True)


def to_row(eye, x):
    return down(jnp.where(eye, jnp.sum(x, axis=1, keepdims=True), 0.0))


def scale_of(x):
    return lax.rsqrt(down(x * x) + EPSILON)


def local_head(q, k, do, rows):
    c = q.shape[0]
    dv = do.shape[1]
    eye, upper, strict = head_masks(c)
    g, beta, cd, to_end = rows[0:1], rows[1:2], rows[2:3], rows[3:4]
    qt, kt = q.T, k.T
    grams = mm(k, jnp.concatenate([k, q], axis=0), 1, 1)
    yield
    rq, rk = scale_of(qt.astype(F32)), scale_of(kt.astype(F32))
    start = to_col(eye, jnp.log(rk) - g)
    decay = jnp.exp(jnp.where(upper, start + g, -1e30))
    kk = grams[:, :c]
    pt = decay * rq * grams[:, c:]
    pairs = jnp.where(strict, decay, 0.0) * rk
    ptdo = mm(pt, do).astype(BF)
    inv = yield from inverse(beta * pairs * kk)
    left = jnp.concatenate([inv.astype(BF), (inv * (to_end * rk)).astype(BF)], axis=1)
    right = jnp.concatenate(
        [
            jnp.concatenate([ptdo, jnp.zeros(k.shape, BF)], axis=1),
            jnp.concatenate([jnp.zeros(do.shape, BF), k], axis=1),
        ],
        axis=0,
    )
    both = mm(left, right)
    yield
    left = jnp.concatenate(
        [(qt * (cd * rq)).astype(BF), (kt * (-beta * cd * rk)).astype(BF)], axis=1
    )
    right = jnp.concatenate(
        [jnp.concatenate([do, jnp.zeros(k.shape, BF)], axis=1), both.astype(BF)], axis=0
    )
    made = mm(left, right)
    yield
    return qt, kt, rq, rk, decay, pairs, kk, pt, inv, both[:, :dv], both[:, dv:], made


def local_rest(k, v, do, s0, rows, qt, kt, rq, rk, decay, pt, inv):
    c = k.shape[0]
    eye, _, _ = head_masks(c)
    beta, cd = rows[1:2], rows[2:3]
    sb = s0.astype(BF)
    ks = mm(k, sb)
    back = inv.T
    yield
    left = jnp.concatenate([back * beta, back * (-beta * cd * rk)], axis=1)
    ub = mm(left, jnp.concatenate([v, ks.astype(BF)], axis=0)).astype(BF)
    yield
    prod = mm(jnp.concatenate([ub, sb], axis=0), do, 1, 1)
    yield
    dpt, dost = prod[:c], prod[c:] * cd
    t = dpt * pt
    gdp = (decay * dpt).astype(BF)
    qn = qt * rq
    dqk = mm(kt, gdp)
    dk0 = mm(qn, gdp, 1, 1)
    yield
    dg0 = down(t) + down(dost * qn) - to_row(eye, t)
    dqn = rq * (dost + dqk)
    dq = dqn - qn * down(qn * dqn)
    yield
    return dq.astype(BF).T, ks, ub, dk0, dg0


def carry_head(v, s0, e, rows, kt, rk, pairs, kk, ub, w0, nb, ks, dk0, dg0):
    c = v.shape[0]
    eye, _, _ = head_masks(c)
    beta, cd, to_end = rows[1:2], rows[2:3], rows[3:4]
    w = w0 + mm(nb, e)
    ue = mm(e, ub, 1, 1)
    yield
    wb = w.astype(BF)
    prod = mm(jnp.concatenate([ub, s0.astype(BF)], axis=0), wb, 1, 1)
    ue = (to_end * rk) * ue
    s = down(kt * ue)
    wv = to_row(eye, w * v.astype(F32))
    wks = (cd * rk) * to_row(eye, w * ks)
    yield
    da = -prod[:c] * pairs
    pair = (beta * da).astype(BF)
    kn = kt * rk
    dkn = dk0 - (beta * cd * rk) * prod[c:] + ue
    near, far = mm(kt, pair), mm(kt, pair, 1, 1)
    da = da * kk
    own = down(da)
    dbeta = own + wv - wks
    dg = dg0 + beta * (own - wks) - to_row(eye, beta * da) - s
    yield
    dkn = dkn + near + far
    dk = dkn - kn * down(kn * dkn)
    last = cd[:, c - 1 :]
    tail = jnp.sum(s, keepdims=True) + last * jnp.sum(down(s0 * e.astype(F32)), keepdims=True)
    lane = lax.broadcasted_iota(jnp.int32, (1, c), 1)
    dg = dg + jnp.where(lane == c - 1, tail, 0.0)
    dv = to_col(eye, beta) * w
    yield
    return dv, dk.astype(BF).T, dg, dbeta


def split3(x):
    hi = x.astype(BF)
    rest = x - hi.astype(F32)
    mid = rest.astype(BF)
    return hi, mid, (rest - mid.astype(F32)).astype(BF)


def group_size(n, heads):
    size = 1
    while (2 * size) ** 2 <= n and heads % (2 * size) == 0 and n % (2 * size) == 0:
        size *= 2
    return size


def middle_planes(planes):
    low = planes // 4
    return low, planes - 2 * low


def whole_kernel(
    n, m, size,
    q_in, k_in, v_in, do_in, s0_in, hidden_in, decay_w_in, write_w_in,
    decay_bias_in, decay_log_in, write_bias_in,
    dq_out, dk_out, dv_out, gh, gd, gw,
    q_raw, k_raw, v_raw, do_raw, s0, hidden, decay_w, write_w, decay_bias, decay_log, write_bias,
    q, k, v, do, dq, dk, dv, rows, fac, weights, qts, kts, scales, decay, pairs, kks, pts, invs, w0, nb, ks, ub, dk0, dg0, dgs, dbs,
    ends, ends_in, maps, maps_in, tcomp, bcomp, gcomp, far_out, far_in, zin, zout, eout, ein,
    tbuf, got, part, gathered, ggot, wgot,
    in_sems, far_sems, end_sems, map_sems, map_recv, z_sems, e_send, e_recv, sum_sems, head_sems,
):
    me, side = lax.axis_index("seq"), lax.axis_index("head")
    mesh_id = pl.DeviceIdType.MESH
    heads, c, dkk = q.shape
    dvv = v.shape[2]
    own = heads // size
    planes = n // size
    plane, rank = me // size, lax.rem(me, size)
    lag = planes - 1 - plane
    direct = min(own, 2)
    chained = own - direct
    barrier = pltpu.get_barrier_semaphore()

    def run(low, high, body):
        def step(d, _):
            body(d)
            return 0

        lax.fori_loop(low, high, step, 0)

    def ahead(d):
        return lax.rem(me + d, n)

    def behind(d):
        return lax.rem(me + n - d, n)

    def side_ahead(d):
        return lax.rem(side + d, m)

    def side_behind(d):
        return lax.rem(side + m - d, m)

    def far_first(d):
        skip = jnp.where(plane < planes // 2, planes - 1 - d // size, d // size)
        return skip * size + lax.rem(rank + 1 + d, size)

    def to_all(start):
        def one(d):
            to = far_first(d)

            @pl.when(to != me)
            def _():
                start(to)

        run(0, n, one)

    def greet(d):
        pl.semaphore_signal(barrier, inc=1, device_id={"seq": ahead(d)}, device_id_type=mesh_id)

    def greet_side(d):
        pl.semaphore_signal(
            barrier, inc=1, device_id={"head": side_ahead(d)}, device_id_type=mesh_id
        )

    arrays = (
        (hidden_in, hidden), (decay_w_in, decay_w), (write_w_in, write_w),
        (decay_bias_in, decay_bias), (decay_log_in, decay_log), (write_bias_in, write_bias),
        (k_in, k_raw), (q_in, q_raw), (do_in, do_raw), (v_in, v_raw), (s0_in, s0),
    )
    loads = [pltpu.make_async_copy(a, b, in_sems.at[i]) for i, (a, b) in enumerate(arrays)]
    for load in loads:
        load.start()

    run(1, n, greet)
    run(1, m, greet_side)
    width = hidden.shape[1]
    low, count = middle_planes(planes)
    base, adders = low * size, count * size
    w = width // adders
    seat = me - base
    adding = (seat >= 0) & (seat < adders)

    def send_map(b, to, source):
        return pltpu.make_async_remote_copy(
            src_ref=maps.at[b, to], dst_ref=maps_in.at[b, source],
            send_sem=map_sems.at[b, to], recv_sem=map_recv.at[b, source],
            device_id={"seq": plane * size + to}, device_id_type=mesh_id,
        )

    def send_ends(to, source):
        return pltpu.make_async_remote_copy(
            src_ref=ends, dst_ref=ends_in.at[source],
            send_sem=end_sems.at[0, to], recv_sem=end_sems.at[1, source],
            device_id={"seq": plane * size + to}, device_id_type=mesh_id,
        )

    def send_plane(b):
        return pltpu.make_async_remote_copy(
            src_ref=zout.at[b], dst_ref=zin.at[b],
            send_sem=z_sems.at[0, b], recv_sem=z_sems.at[1, b],
            device_id={"seq": lax.rem(me + n - size, n)}, device_id_type=mesh_id,
        )

    def send_far(i, to, source, part):
        return pltpu.make_async_remote_copy(
            src_ref=far_out.at[(i,) + part], dst_ref=far_in.at[(i, source) + part],
            send_sem=far_sems.at[0, i, to], recv_sem=far_sems.at[1, i, source],
            device_id={"seq": to * size + rank}, device_id_type=mesh_id,
        )

    whole_map = (pl.ds(0, dkk + 16), pl.ds(0, dvv + dkk))
    offset_only = (pl.ds(0, dkk), pl.ds(0, dvv))

    def send_back(b, to, owner):
        return pltpu.make_async_remote_copy(
            src_ref=eout.at[b, to], dst_ref=ein.at[owner * own + b],
            send_sem=e_send.at[b, to], recv_sem=e_recv.at[owner * own + b],
            device_id={"seq": plane * size + to}, device_id_type=mesh_id,
        )

    def scatter(to, source):
        return pltpu.make_async_remote_copy(
            src_ref=tbuf.at[to], dst_ref=got.at[source],
            send_sem=sum_sems.at[0, to], recv_sem=sum_sems.at[1, source],
            device_id={"seq": base + to}, device_id_type=mesh_id,
        )

    def gather(to, source):
        return pltpu.make_async_remote_copy(
            src_ref=part, dst_ref=gathered.at[source],
            send_sem=sum_sems.at[2, to], recv_sem=sum_sems.at[3, source],
            device_id={"seq": to}, device_id_type=mesh_id,
        )

    def send_weights(to, source):
        return pltpu.make_async_remote_copy(
            src_ref=weights.at[to], dst_ref=wgot.at[source],
            send_sem=head_sems.at[0, to], recv_sem=head_sems.at[1, source],
            device_id={"head": to}, device_id_type=mesh_id,
        )

    def send_grads(to, source):
        return pltpu.make_async_remote_copy(
            src_ref=ggot.at[side], dst_ref=ggot.at[source],
            send_sem=head_sems.at[2, to], recv_sem=head_sems.at[3, source],
            device_id={"head": to}, device_id_type=mesh_id,
        )

    @pl.when(lag == 0)
    def _():
        zin[...] = jnp.zeros(zin.shape, BF)

    def prepare():
        eye = head_masks(heads)[0]
        for i in range(m):
            cut = pl.ds(i * (width // m), width // m)
            weights[i] = jnp.concatenate([decay_w[:, cut], write_w[:, cut]], axis=0)
        logits = mm(jnp.concatenate([decay_w[...], write_w[...]], axis=0), hidden[...], 1, 1)
        pre = logits[:heads] + to_col(eye, decay_bias[...])
        rate = jnp.exp(to_col(eye, decay_log[...]))
        beta = jax.nn.sigmoid(logits[heads:] + to_col(eye, write_bias[...]))
        log_decay = -rate * (jnp.maximum(pre, 0.0) + jnp.log1p(jnp.exp(-jnp.abs(pre))))
        row, col = indices(c)
        tri = jnp.where(row <= col, 1.0, 0.0).astype(BF)
        sums = mm(jnp.concatenate(split3(log_decay), axis=0), tri)
        g = sums[:heads] + sums[heads : 2 * heads] + sums[2 * heads :]
        fac[:heads] = -rate * jax.nn.sigmoid(pre)
        fac[heads:] = beta * (1.0 - beta)
        parts = (g, beta, jnp.exp(g), jnp.exp(g[:, c - 1 :] - g))
        ends[...] = jnp.broadcast_to(parts[2][:, c - 1 :], ends.shape)
        ends_in[rank] = jnp.broadcast_to(parts[2][:, c - 1 :], ends.shape)
        for h in range(heads):
            for i, a in enumerate(parts):
                rows[h, i : i + 1] = a[h : h + 1]

    def wait_barrier():
        pl.semaphore_wait(barrier, n + m - 2)

    def batch_heads(b):
        return [j * own + b for j in range(size)]

    def local_parts(b):
        return [local_head(q[h], k[h], do[h], rows[h]) for h in batch_heads(b)]

    def local_store(b, outs):
        for j, h in enumerate(batch_heads(b)):
            qts[h], kts[h], rq, rk, decay[h], pairs[h], kks[h], pts[h], inv, w0_, nb_, made = outs[j]
            scales[h, 0:1] = rq
            scales[h, 1:2] = rk
            invs[h], w0[h], nb[h] = inv.astype(BF), w0_, nb_.astype(BF)
            maps[b, j] = made.astype(BF)

    def rest_parts(b):
        return [
            local_rest(
                k[h], v[h], do[h], s0[h], rows[h], qts[h], kts[h],
                scales[h, 0:1], scales[h, 1:2], decay[h], pts[h], invs[h],
            )
            for h in batch_heads(b)
        ]

    def rest_store(b, outs):
        for j, h in enumerate(batch_heads(b)):
            dq[h], ks[h], ub[h], dk0[h], dg0[h] = outs[j]

    def local_batch(b):
        local_store(b, lockstep((local_parts(b), 1))[0])

    def rest_batch(b):
        rest_store(b, lockstep((rest_parts(b), 1))[0])

    def both_batches(s):
        outs = lockstep((rest_parts(s - 1), 2), (local_parts(s), 1))
        rest_store(s - 1, outs[0])
        local_store(s, outs[1])

    def end_sends():
        for j in range(size):

            @pl.when(rank != j)
            def _():
                send_ends(j, rank).start()

    def wait_ends():
        for p in range(size):

            @pl.when(rank != p)
            def _():
                send_ends(p, p).wait_recv()

    def local_sends(b):
        for j in range(size):

            @pl.when(rank != j)
            def _():
                send_map(b, j, rank).start()

        maps_in[b, rank] = maps[b, rank]

    def piece(b, p):
        return maps_in[b, p], ends_in[p, pl.ds(rank * own + b, 1), :]

    def wait_maps(b):
        for p in range(size):

            @pl.when(rank != p)
            def _():
                send_map(b, p, p).wait_recv()

    def compose(b):
        wait_maps(b)
        @pl.when(lag == 0)
        def _():
            both = maps_in[b, size - 1, :, :dvv].astype(F32)
            for p in range(size - 2, -1, -1):
                made, last = piece(b, p)
                prod = mm(made[:, dvv:], both)
                both = last[:, :1] * both + made[:, :dvv].astype(F32) + prod
            bcomp[b] = both

        @pl.when((lag > 0) & (plane > 0))
        def _():
            made, g = piece(b, size - 1)
            both = made.astype(F32)
            for p in range(size - 2, -1, -1):
                made, last = piece(b, p)
                step = made.astype(F32)
                prod = mm(made[:, dvv:], both)
                both = last[:, :1] * both + jnp.concatenate(
                    [step[:, :dvv], g[:, :1] * step[:, dvv:]], axis=1
                ) + prod
                g = last * g
            bcomp[b] = both[:, :dvv]
            tcomp[b] = both[:, dvv:].astype(BF)
            gcomp[b] = jnp.broadcast_to(g, gcomp.shape[1:])

    def wait_plane(b):
        send_plane(b).wait_recv()

    def hand_on(b):
        @pl.when((lag == 0) & (plane > 0))
        def _():
            zout[b] = bcomp[b].astype(BF)

        @pl.when(lag > 0)
        def _():
            wait_plane(b)

            @pl.when(plane > 0)
            def _():
                eb = zin[b]
                e = gcomp[b, 0:1] * eb.astype(F32) + bcomp[b] + mm(tcomp[b], eb)
                zout[b] = e.astype(BF)

        @pl.when(plane > 0)
        def _():
            send_plane(b).start()

    def send_fars(b):
        i = b - chained

        @pl.when(lag == 0)
        def _():
            far_out[i, :dkk, :dvv] = bcomp[b].astype(BF)
            run(0, plane, lambda p: send_far(i, p, plane, offset_only).start())

        @pl.when(lag > 0)
        def _():
            g = gcomp[b]
            high = g.astype(BF)
            low = (g - high.astype(F32)).astype(BF)
            far_out[i, :dkk] = jnp.concatenate([bcomp[b].astype(BF), tcomp[b]], axis=1)
            far_out[i, dkk : dkk + 8, :dvv] = high
            far_out[i, dkk + 8 :, :dvv] = low
            run(0, plane, lambda p: send_far(i, p, plane, whole_map).start())

    def resolve(b):
        i = b - chained
        send_far(i, planes - 1, planes - 1, offset_only).wait_recv()

        def fold(d, e):
            source = planes - 2 - d
            send_far(i, source, source, whole_map).wait_recv()
            made = far_in[i, source, :dkk]
            g = far_in[i, source, dkk:, :dvv].astype(F32)
            prod = mm(made[:, dvv:], e)
            return (g[0:1] + g[8:9]) * e + made[:, :dvv].astype(F32) + prod

        e = far_in[i, planes - 1, :dkk, :dvv].astype(F32)
        zin[b] = lax.fori_loop(0, lag - 1, fold, e).astype(BF)

    def hand_back(b):
        eb = zin[b]
        e = eb.astype(F32)
        for p in range(size - 1, -1, -1):
            eout[b, p] = eb

            @pl.when(rank == p)
            def _():
                ein[rank * own + b] = eb

            @pl.when(rank != p)
            def _():
                send_back(b, p, rank).start()

            if p > 0:
                made, last = piece(b, p)
                e = last * e + made[:, :dvv].astype(F32) + mm(made[:, dvv:], eb)
                eb = e.astype(BF)

    def wait_back(b):
        for j in range(size):

            @pl.when(rank != j)
            def _():
                send_back(b, rank, j).wait_recv()

    def carry_batch(b):
        wait_back(b)
        parts = [
            carry_head(
                v[h], s0[h], ein[h], rows[h], kts[h], scales[h, 1:2], pairs[h], kks[h], ub[h],
                w0[h], nb[h], ks[h], dk0[h], dg0[h],
            )
            for h in batch_heads(b)
        ]
        outs = lockstep((parts, 1))[0]
        for j, h in enumerate(batch_heads(b)):
            dv[h] = outs[j][0].astype(BF)
            dk[h] = outs[j][1]
            dgs[pl.ds(h, 1), :] = outs[j][2]
            dbs[pl.ds(h, 1), :] = outs[j][3]

    late = max(own, planes) + 2


    def first_batch():
        local_batch(0)
        wait_barrier()
        run(1, m, lambda d: send_weights(side_ahead(d), side).start())
        end_sends()
        local_sends(0)

    def pass_on(s):
        turn = s - 1 - lag

        @pl.when((lag > 0) & (turn >= 0) & (turn < chained))
        def _():
            hand_on(turn)

        @pl.when((lag > 0) & (turn >= chained) & (turn < own))
        def _():
            resolve(turn)

    def gather_maps(s):
        @pl.when(s == 1)
        def _():
            wait_ends()

        compose(s - 1)

        @pl.when((lag == 0) & (s <= chained))
        def _():
            hand_on(s - 1)

        @pl.when((plane > 0) & (s > chained))
        def _():
            send_fars(s - 1)

    def early(s):
        both_batches(s)
        local_sends(s)
        pass_on(s)
        gather_maps(s)

    def middle():
        pass_on(own)
        rest_batch(own - 1)
        gather_maps(own)
        run(0, jnp.maximum(own - lag, 0), hand_back)

    def later(s):
        pass_on(s)
        turn = s - 1 - lag

        @pl.when((turn >= 0) & (turn < own))
        def _():
            hand_back(turn)

        @pl.when(s >= late)
        def _():
            carry_batch(s - late)

    def take(first, last, pairs):
        for load in loads[first:last]:
            load.wait()
        for ref, raw in pairs:
            ref[...] = jnp.swapaxes(raw[...], 0, 1)

    take(0, 6, ())
    prepare()
    take(6, 9, ((k, k_raw), (q, q_raw), (do, do_raw)))
    first_batch()
    take(9, 11, ((v, v_raw),))
    run(1, own, early)
    middle()
    run(own + 1, own + late, later)

    def finish_grads():
        row, col = indices(c)
        tri = jnp.where(row >= col, 1.0, 0.0).astype(BF)
        sums = mm(jnp.concatenate(split3(dgs[...]), axis=0), tri)
        dlog = sums[:heads] + sums[heads : 2 * heads] + sums[2 * heads :]
        grads = jnp.concatenate([dlog * fac[:heads], dbs[...] * fac[heads:]], axis=0).astype(BF)
        ggot[side] = grads
        run(1, m, lambda d: send_grads(side_ahead(d), side).start())
        return grads

    def weight_terms(grads):
        terms = mm(grads, hidden[...])
        for i in range(adders):
            tbuf[i] = terms[:, i * w : (i + 1) * w].astype(BF)

        def give(to):
            @pl.when((to >= base) & (to < base + adders))
            def _():
                scatter(to - base, me).start()

        to_all(give)

    def partner(d):
        source = side_behind(d)
        send_weights(source, source).wait_recv()
        send_grads(source, source).wait_recv()

    def input_grad():
        wgot[side] = weights[side]
        run(1, m, partner)
        total = mm(ggot[0], wgot[0], 0, 0)
        for i in range(1, m):
            total = total + mm(ggot[i], wgot[i], 0, 0)
        gh[...] = total.astype(BF)

    def reduce_terms():
        def add(d, acc):
            source = behind(d)
            scatter(seat, source).wait_recv()
            return acc + got[source].astype(F32)

        @pl.when(adding)
        def _():
            acc = lax.fori_loop(1, n, add, tbuf[seat].astype(F32)).astype(BF)
            part[...] = acc
            gathered[seat] = acc
            to_all(lambda to: gather(to, seat).start())

    def arrivals():
        def arrive(i):
            @pl.when(i != seat)
            def _():
                gather(base, i).wait_recv()

        run(0, adders, arrive)

    def reorder():
        for ref, source in ((dq_out, dq), (dk_out, dk), (dv_out, dv)):
            ref[...] = jnp.swapaxes(source[...], 0, 1)

    def write_sums():
        for i in range(adders):
            both = gathered[i].astype(F32)
            gd[:, i * w : (i + 1) * w] = both[:heads]
            gw[:, i * w : (i + 1) * w] = both[heads:]

    def done(b):
        for j in range(size):

            @pl.when(rank != j)
            def _():
                send_map(b, j, rank).wait_send()
                send_back(b, j, rank).wait_send()

        @pl.when((plane > 0) & (b < chained))
        def _():
            send_plane(b).wait_send()

        @pl.when((b >= chained) & (lag == 0))
        def _():
            run(0, plane, lambda p: send_far(b - chained, p, plane, offset_only).wait_send())

        @pl.when((b >= chained) & (lag > 0))
        def _():
            run(0, plane, lambda p: send_far(b - chained, p, plane, whole_map).wait_send())

    weight_terms(finish_grads())
    input_grad()
    reduce_terms()
    reorder()
    arrivals()
    write_sums()
    for j in range(size):

        @pl.when(rank != j)
        def _():
            send_ends(j, rank).wait_send()

    run(0, own, done)
    def given(i):
        @pl.when(i != seat)
        def _():
            scatter(i, me).wait_send()

    run(0, adders, given)

    @pl.when(adding)
    def _():
        run(1, n, lambda d: gather(ahead(d), seat).wait_send())

    run(1, m, lambda d: send_weights(side_ahead(d), side).wait_send())
    run(1, m, lambda d: send_grads(side_ahead(d), side).wait_send())


def whole_part(n, m, q, k, v, do, s0, hidden, *gates):
    c, h, dk = q.shape
    dv = v.shape[2]
    size = group_size(n, h)
    own = h // size
    width = hidden.shape[1]
    adders = middle_planes(n // size)[1] * size
    w = width // adders
    vm = pl.BlockSpec(memory_space=pltpu.VMEM)
    sd = jax.ShapeDtypeStruct
    dma = pltpu.SemaphoreType.DMA
    message = (dk, dv + dk)
    return pl.pallas_call(
        partial(whole_kernel, n, m, size),
        out_shape=(
            pltpu.VMEM((c, h, dk), BF), pltpu.VMEM((c, h, dk), BF), pltpu.VMEM((c, h, dv), BF), pltpu.VMEM((c, width // m), BF),
            pltpu.VMEM((h, width), F32), pltpu.VMEM((h, width), F32),
        ),
        in_specs=[pl.BlockSpec(memory_space=pl.ANY)] * 11,
        out_specs=(vm,) * 6,
        scratch_shapes=[pltpu.VMEM(a.shape, a.dtype) for a in (q, k, v, do, s0, hidden) + gates]
        + [
            pltpu.VMEM((h, c, dk), BF), pltpu.VMEM((h, c, dk), BF), pltpu.VMEM((h, c, dv), BF),
            pltpu.VMEM((h, c, dv), BF),
            pltpu.VMEM((h, c, dk), BF), pltpu.VMEM((h, c, dk), BF), pltpu.VMEM((h, c, dv), BF),
            pltpu.VMEM((h, 8, c), F32), pltpu.VMEM((2 * h, c), F32),
            pltpu.VMEM((m, 2 * h, width // m), BF),
            pltpu.VMEM((h, dk, c), BF), pltpu.VMEM((h, dk, c), BF), pltpu.VMEM((h, 8, c), F32),
            pltpu.VMEM((h, c, c), F32), pltpu.VMEM((h, c, c), F32), pltpu.VMEM((h, c, c), F32),
            pltpu.VMEM((h, c, c), F32), pltpu.VMEM((h, c, c), BF), pltpu.VMEM((h, c, dv), F32),
            pltpu.VMEM((h, c, dk), BF), pltpu.VMEM((h, c, dv), F32), pltpu.VMEM((h, c, dv), BF),
            pltpu.VMEM((h, dk, c), F32),
            pltpu.VMEM((h, 1, c), F32), pltpu.VMEM((h, c), F32), pltpu.VMEM((h, c), F32),
            pltpu.VMEM((h, dv), F32), pltpu.VMEM((size, h, dv), F32),
            pltpu.VMEM((own, size) + message, BF), pltpu.VMEM((own, size) + message, BF),
            pltpu.VMEM((own, dk, dk), BF), pltpu.VMEM((own, dk, dv), F32),
            pltpu.VMEM((own, 8, dv), F32),
            pltpu.VMEM((min(own, 2), dk + 16, dv + dk), BF),
            pltpu.VMEM((min(own, 2), n // size, dk + 16, dv + dk), BF),
            pltpu.VMEM((own, dk, dv), BF), pltpu.VMEM((own, dk, dv), BF),
            pltpu.VMEM((own, size, dk, dv), BF), pltpu.VMEM((h, dk, dv), BF),
            pltpu.VMEM((adders, 2 * h, w), BF), pltpu.VMEM((n, 2 * h, w), BF),
            pltpu.VMEM((2 * h, w), BF), pltpu.VMEM((adders, 2 * h, w), BF),
            pltpu.VMEM((m, 2 * h, c), BF), pltpu.VMEM((m, 2 * h, width // m), BF),
            dma((11,)), dma((2, min(own, 2), n // size)), dma((2, size)), dma((own, size)), dma((own, size)), dma((2, own)), dma((own, size)), dma((h,)),
            dma((4, n)), dma((4, m)),
        ],
        compiler_params=pltpu.CompilerParams(
            collective_id=0, has_side_effects=True, vmem_limit_bytes=57000 * 1024
        ),
    )(q, k, v, do, s0, hidden, *gates)


def store_kernel(*refs):
    count = (len(refs) - 1) // 2
    sems = refs[-1]
    copies = [
        pltpu.make_async_copy(refs[i], refs[count + i], sems.at[i]) for i in range(count)
    ]
    for copy in copies:
        copy.start()
    for copy in copies:
        copy.wait()


def store_part(arrays):
    count = len(arrays)
    return pl.pallas_call(
        store_kernel,
        out_shape=tuple(jax.ShapeDtypeStruct(a.shape, a.dtype) for a in arrays),
        in_specs=[pl.BlockSpec(memory_space=pltpu.VMEM)] * count,
        out_specs=(pl.BlockSpec(memory_space=pl.ANY),) * count,
        scratch_shapes=[pltpu.SemaphoreType.DMA((count,))],
        compiler_params=pltpu.CompilerParams(vmem_limit_bytes=8 * 1024 * 1024),
    )(*arrays)


def shards(
    queries,
    key_vectors,
    values,
    out_grad,
    hidden_in,
    decay_weight,
    write_weight,
    decay_bias,
    decay_log,
    write_bias,
    start_state,
):
    n, m = lax.axis_size("seq"), lax.axis_size("head")
    made = whole_part(
        n, m, queries, key_vectors, values, out_grad, start_state[0], hidden_in, decay_weight.T, write_weight.T,
        decay_bias[None], decay_log[None], write_bias[None],
    )
    dq, dk, dv, gh, gd, gw = store_part(made)
    return dq, dk, dv, gh, gd.T, gw.T


def solution(mesh):
    placed = (
        P("seq", "head", None),
        P("seq", "head", None),
        P("seq", "head", None),
        P("seq", "head", None),
        P("seq", None),
        P(None, "head"),
        P(None, "head"),
        P("head"),
        P("head"),
        P("head"),
        P("seq", "head", None, None),
    )
    return jax.shard_map(
        shards,
        mesh=mesh,
        in_specs=placed,
        out_specs=(
            P("seq", "head", None),
            P("seq", "head", None),
            P("seq", "head", None),
            P("seq", "head"),
            P(None, "head"),
            P(None, "head"),
        ),
        check_vma=False,
    )
```

```python
from functools import partial

import jax
import jax.numpy as jnp
from jax import lax
from jax.experimental import pallas as pl
from jax.experimental.pallas import tpu as pltpu
from jax.sharding import PartitionSpec as P

EPSILON = 1e-06
F32 = jnp.float32
BF = jnp.bfloat16


def mm(a, b, ca=1, cb=0):
    return lax.dot_general(
        a.astype(BF), b.astype(BF), (((ca,), (cb,)), ((), ())), preferred_element_type=F32
    )


def indices(c):
    row = lax.broadcasted_iota(jnp.int32, (c, c), 0)
    col = lax.broadcasted_iota(jnp.int32, (c, c), 1)
    return row, col


def lockstep(*groups):
    results = [[None] * len(members) for members, _ in groups]
    active = {(i, j) for i, (members, _) in enumerate(groups) for j in range(len(members))}
    tick = 0
    while active:
        for i, (members, period) in enumerate(groups):
            for j, member in enumerate(members):
                if (i, j) in active and tick % period == 0:
                    try:
                        next(member)
                    except StopIteration as end:
                        results[i][j] = end.value
                        active.remove((i, j))
        tick += 1
    return results


def inverse(a):
    c = a.shape[0]
    row, col = indices(c)
    inv = jnp.where(row == col, 1.0, jnp.where((row ^ col) == 1, -a, 0.0))
    level = 1
    while (2 << level) <= c:
        near = ((row >> level) ^ (col >> level)) == 1
        half = mm(inv, jnp.where(near, a, 0.0))
        yield
        step = mm(half, inv)
        yield
        inv = inv - step
        level += 1
    return inv


def head_masks(c):
    row, col = indices(c)
    return row == col, col >= row, col > row


def down(x):
    return jnp.sum(x, axis=0, keepdims=True)


def to_col(eye, row):
    return jnp.sum(jnp.where(eye, row, 0.0), axis=1, keepdims=True)


def to_row(eye, x):
    return down(jnp.where(eye, jnp.sum(x, axis=1, keepdims=True), 0.0))


def scale_of(x):
    return lax.rsqrt(down(x * x) + EPSILON)


def local_head(q, k, do, rows):
    c = q.shape[0]
    dv = do.shape[1]
    eye, upper, strict = head_masks(c)
    g, beta, cd, to_end = rows[0:1], rows[1:2], rows[2:3], rows[3:4]
    qt, kt = q.T, k.T
    grams = mm(k, jnp.concatenate([k, q], axis=0), 1, 1)
    yield
    rq, rk = scale_of(qt.astype(F32)), scale_of(kt.astype(F32))
    start = to_col(eye, jnp.log(rk) - g)
    decay = jnp.exp(jnp.where(upper, start + g, -1e30))
    kk = grams[:, :c]
    pt = decay * rq * grams[:, c:]
    pairs = jnp.where(strict, decay, 0.0) * rk
    ptdo = mm(pt, do).astype(BF)
    inv = yield from inverse(beta * pairs * kk)
    left = jnp.concatenate([inv.astype(BF), (inv * (to_end * rk)).astype(BF)], axis=1)
    right = jnp.concatenate(
        [
            jnp.concatenate([ptdo, jnp.zeros(k.shape, BF)], axis=1),
            jnp.concatenate([jnp.zeros(do.shape, BF), k], axis=1),
        ],
        axis=0,
    )
    both = mm(left, right)
    yield
    left = jnp.concatenate(
        [(qt * (cd * rq)).astype(BF), (kt * (-beta * cd * rk)).astype(BF)], axis=1
    )
    right = jnp.concatenate(
        [jnp.concatenate([do, jnp.zeros(k.shape, BF)], axis=1), both.astype(BF)], axis=0
    )
    made = mm(left, right)
    yield
    return qt, kt, rq, rk, decay, pairs, kk, pt, inv, both[:, :dv], both[:, dv:], made


def local_rest(k, v, do, s0, rows, qt, kt, rq, rk, decay, pt, inv):
    c = k.shape[0]
    eye, _, _ = head_masks(c)
    beta, cd = rows[1:2], rows[2:3]
    sb = s0.astype(BF)
    ks = mm(k, sb)
    back = inv.T
    yield
    left = jnp.concatenate([back * beta, back * (-beta * cd * rk)], axis=1)
    ub = mm(left, jnp.concatenate([v, ks.astype(BF)], axis=0)).astype(BF)
    yield
    prod = mm(jnp.concatenate([ub, sb], axis=0), do, 1, 1)
    yield
    dpt, dost = prod[:c], prod[c:] * cd
    t = dpt * pt
    gdp = (decay * dpt).astype(BF)
    qn = qt * rq
    dqk = mm(kt, gdp)
    dk0 = mm(qn, gdp, 1, 1)
    yield
    dg0 = down(t) + down(dost * qn) - to_row(eye, t)
    dqn = rq * (dost + dqk)
    dq = dqn - qn * down(qn * dqn)
    yield
    return dq.astype(BF).T, ks, ub, dk0, dg0


def carry_head(v, s0, e, rows, kt, rk, pairs, kk, ub, w0, nb, ks, dk0, dg0):
    c = v.shape[0]
    eye, _, _ = head_masks(c)
    beta, cd, to_end = rows[1:2], rows[2:3], rows[3:4]
    w = w0 + mm(nb, e)
    ue = mm(e, ub, 1, 1)
    yield
    wb = w.astype(BF)
    prod = mm(jnp.concatenate([ub, s0.astype(BF)], axis=0), wb, 1, 1)
    ue = (to_end * rk) * ue
    s = down(kt * ue)
    wv = to_row(eye, w * v.astype(F32))
    wks = (cd * rk) * to_row(eye, w * ks)
    yield
    da = -prod[:c] * pairs
    pair = (beta * da).astype(BF)
    kn = kt * rk
    dkn = dk0 - (beta * cd * rk) * prod[c:] + ue
    near, far = mm(kt, pair), mm(kt, pair, 1, 1)
    da = da * kk
    own = down(da)
    dbeta = own + wv - wks
    dg = dg0 + beta * (own - wks) - to_row(eye, beta * da) - s
    yield
    dkn = dkn + near + far
    dk = dkn - kn * down(kn * dkn)
    last = cd[:, c - 1 :]
    tail = jnp.sum(s, keepdims=True) + last * jnp.sum(down(s0 * e.astype(F32)), keepdims=True)
    lane = lax.broadcasted_iota(jnp.int32, (1, c), 1)
    dg = dg + jnp.where(lane == c - 1, tail, 0.0)
    dv = to_col(eye, beta) * w
    yield
    return dv, dk.astype(BF).T, dg, dbeta


def split3(x):
    hi = x.astype(BF)
    rest = x - hi.astype(F32)
    mid = rest.astype(BF)
    return hi, mid, (rest - mid.astype(F32)).astype(BF)


def group_size(n, heads):
    size = 1
    while (2 * size) ** 2 <= n and heads % (2 * size) == 0 and n % (2 * size) == 0:
        size *= 2
    return size


def middle_planes(planes):
    low = planes // 4
    return low, planes - 2 * low


def whole_kernel(
    n, m, size,
    q_in, k_in, v_in, do_in, s0_in, hidden_in, decay_w_in, write_w_in,
    decay_bias_in, decay_log_in, write_bias_in,
    dq_out, dk_out, dv_out, gh, gd, gw,
    q_raw, k_raw, v_raw, do_raw, s0, hidden, decay_w, write_w, decay_bias, decay_log, write_bias,
    q, k, v, do, dq, dk, dv, rows, fac, weights, qts, kts, scales, decay, pairs, kks, pts, invs, w0, nb, ks, ub, dk0, dg0, dgs, dbs,
    ends, ends_in, maps, maps_in, tcomp, bcomp, gcomp, far_out, far_in, zin, zout, eout, ein,
    tbuf, got, part, gathered, ggot, wgot,
    in_sems, far_sems, end_sems, map_sems, map_recv, z_sems, e_send, e_recv, sum_sems, head_sems,
):
    me, side = lax.axis_index("seq"), lax.axis_index("head")
    mesh_id = pl.DeviceIdType.MESH
    heads, c, dkk = q.shape
    dvv = v.shape[2]
    own = heads // size
    planes = n // size
    plane, rank = me // size, lax.rem(me, size)
    lag = planes - 1 - plane
    direct = min(own, 2)
    chained = own - direct
    barrier = pltpu.get_barrier_semaphore()

    def run(low, high, body):
        def step(d, _):
            body(d)
            return 0

        lax.fori_loop(low, high, step, 0)

    def ahead(d):
        return lax.rem(me + d, n)

    def behind(d):
        return lax.rem(me + n - d, n)

    def side_ahead(d):
        return lax.rem(side + d, m)

    def side_behind(d):
        return lax.rem(side + m - d, m)

    def far_first(d):
        skip = jnp.where(plane < planes // 2, planes - 1 - d // size, d // size)
        return skip * size + lax.rem(rank + 1 + d, size)

    def to_all(start):
        def one(d):
            to = far_first(d)

            @pl.when(to != me)
            def _():
                start(to)

        run(0, n, one)

    def greet(d):
        pl.semaphore_signal(barrier, inc=1, device_id={"seq": ahead(d)}, device_id_type=mesh_id)

    def greet_side(d):
        pl.semaphore_signal(
            barrier, inc=1, device_id={"head": side_ahead(d)}, device_id_type=mesh_id
        )

    arrays = (
        (hidden_in, hidden), (decay_w_in, decay_w), (write_w_in, write_w),
        (decay_bias_in, decay_bias), (decay_log_in, decay_log), (write_bias_in, write_bias),
        (k_in, k_raw), (q_in, q_raw), (do_in, do_raw), (v_in, v_raw), (s0_in, s0),
    )
    loads = [pltpu.make_async_copy(a, b, in_sems.at[i]) for i, (a, b) in enumerate(arrays)]
    for load in loads:
        load.start()

    run(1, n, greet)
    run(1, m, greet_side)
    width = hidden.shape[1]
    low, count = middle_planes(planes)
    base, adders = low * size, count * size
    w = width // adders
    seat = me - base
    adding = (seat >= 0) & (seat < adders)

    def send_map(b, to, source):
        return pltpu.make_async_remote_copy(
            src_ref=maps.at[b, to], dst_ref=maps_in.at[b, source],
            send_sem=map_sems.at[b, to], recv_sem=map_recv.at[b, source],
            device_id={"seq": plane * size + to}, device_id_type=mesh_id,
        )

    def send_ends(to, source):
        return pltpu.make_async_remote_copy(
            src_ref=ends, dst_ref=ends_in.at[source],
            send_sem=end_sems.at[0, to], recv_sem=end_sems.at[1, source],
            device_id={"seq": plane * size + to}, device_id_type=mesh_id,
        )

    def send_plane(b):
        return pltpu.make_async_remote_copy(
            src_ref=zout.at[b], dst_ref=zin.at[b],
            send_sem=z_sems.at[0, b], recv_sem=z_sems.at[1, b],
            device_id={"seq": lax.rem(me + n - size, n)}, device_id_type=mesh_id,
        )

    def send_far(i, to, source, part):
        return pltpu.make_async_remote_copy(
            src_ref=far_out.at[(i,) + part], dst_ref=far_in.at[(i, source) + part],
            send_sem=far_sems.at[0, i, to], recv_sem=far_sems.at[1, i, source],
            device_id={"seq": to * size + rank}, device_id_type=mesh_id,
        )

    whole_map = (pl.ds(0, dkk + 16), pl.ds(0, dvv + dkk))
    offset_only = (pl.ds(0, dkk), pl.ds(0, dvv))

    def send_back(b, to, owner):
        return pltpu.make_async_remote_copy(
            src_ref=eout.at[b, to], dst_ref=ein.at[owner * own + b],
            send_sem=e_send.at[b, to], recv_sem=e_recv.at[owner * own + b],
            device_id={"seq": plane * size + to}, device_id_type=mesh_id,
        )

    def scatter(to, source):
        return pltpu.make_async_remote_copy(
            src_ref=tbuf.at[to], dst_ref=got.at[source],
            send_sem=sum_sems.at[0, to], recv_sem=sum_sems.at[1, source],
            device_id={"seq": base + to}, device_id_type=mesh_id,
        )

    def gather(to, source):
        return pltpu.make_async_remote_copy(
            src_ref=part, dst_ref=gathered.at[source],
            send_sem=sum_sems.at[2, to], recv_sem=sum_sems.at[3, source],
            device_id={"seq": to}, device_id_type=mesh_id,
        )

    def send_weights(to, source):
        return pltpu.make_async_remote_copy(
            src_ref=weights.at[to], dst_ref=wgot.at[source],
            send_sem=head_sems.at[0, to], recv_sem=head_sems.at[1, source],
            device_id={"head": to}, device_id_type=mesh_id,
        )

    def send_grads(to, source):
        return pltpu.make_async_remote_copy(
            src_ref=ggot.at[side], dst_ref=ggot.at[source],
            send_sem=head_sems.at[2, to], recv_sem=head_sems.at[3, source],
            device_id={"head": to}, device_id_type=mesh_id,
        )

    @pl.when(lag == 0)
    def _():
        zin[...] = jnp.zeros(zin.shape, BF)

    def prepare():
        eye = head_masks(heads)[0]
        for i in range(m):
            cut = pl.ds(i * (width // m), width // m)
            weights[i] = jnp.concatenate([decay_w[:, cut], write_w[:, cut]], axis=0)
        logits = mm(jnp.concatenate([decay_w[...], write_w[...]], axis=0), hidden[...], 1, 1)
        pre = logits[:heads] + to_col(eye, decay_bias[...])
        rate = jnp.exp(to_col(eye, decay_log[...]))
        beta = jax.nn.sigmoid(logits[heads:] + to_col(eye, write_bias[...]))
        log_decay = -rate * (jnp.maximum(pre, 0.0) + jnp.log1p(jnp.exp(-jnp.abs(pre))))
        row, col = indices(c)
        tri = jnp.where(row <= col, 1.0, 0.0).astype(BF)
        sums = mm(jnp.concatenate(split3(log_decay), axis=0), tri)
        g = sums[:heads] + sums[heads : 2 * heads] + sums[2 * heads :]
        fac[:heads] = -rate * jax.nn.sigmoid(pre)
        fac[heads:] = beta * (1.0 - beta)
        parts = (g, beta, jnp.exp(g), jnp.exp(g[:, c - 1 :] - g))
        ends[...] = jnp.broadcast_to(parts[2][:, c - 1 :], ends.shape)
        ends_in[rank] = jnp.broadcast_to(parts[2][:, c - 1 :], ends.shape)
        for h in range(heads):
            for i, a in enumerate(parts):
                rows[h, i : i + 1] = a[h : h + 1]

    def wait_barrier():
        pl.semaphore_wait(barrier, n + m - 2)

    def batch_heads(b):
        return [j * own + b for j in range(size)]

    def local_parts(b):
        return [local_head(q[h], k[h], do[h], rows[h]) for h in batch_heads(b)]

    def local_store(b, outs):
        for j, h in enumerate(batch_heads(b)):
            qts[h], kts[h], rq, rk, decay[h], pairs[h], kks[h], pts[h], inv, w0_, nb_, made = outs[j]
            scales[h, 0:1] = rq
            scales[h, 1:2] = rk
            invs[h], w0[h], nb[h] = inv.astype(BF), w0_, nb_.astype(BF)
            maps[b, j] = made.astype(BF)

    def rest_parts(b):
        return [
            local_rest(
                k[h], v[h], do[h], s0[h], rows[h], qts[h], kts[h],
                scales[h, 0:1], scales[h, 1:2], decay[h], pts[h], invs[h],
            )
            for h in batch_heads(b)
        ]

    def rest_store(b, outs):
        for j, h in enumerate(batch_heads(b)):
            dq[h], ks[h], ub[h], dk0[h], dg0[h] = outs[j]

    def local_batch(b):
        local_store(b, lockstep((local_parts(b), 1))[0])

    def rest_batch(b):
        rest_store(b, lockstep((rest_parts(b), 1))[0])

    def both_batches(s):
        outs = lockstep((rest_parts(s - 1), 2), (local_parts(s), 1))
        rest_store(s - 1, outs[0])
        local_store(s, outs[1])

    def end_sends():
        for j in range(size):

            @pl.when(rank != j)
            def _():
                send_ends(j, rank).start()

    def wait_ends():
        for p in range(size):

            @pl.when(rank != p)
            def _():
                send_ends(p, p).wait_recv()

    def local_sends(b):
        for j in range(size):

            @pl.when(rank != j)
            def _():
                send_map(b, j, rank).start()

        maps_in[b, rank] = maps[b, rank]

    def piece(b, p):
        return maps_in[b, p], ends_in[p, pl.ds(rank * own + b, 1), :]

    def wait_maps(b):
        for p in range(size):

            @pl.when(rank != p)
            def _():
                send_map(b, p, p).wait_recv()

    def compose(b):
        wait_maps(b)
        @pl.when(lag == 0)
        def _():
            both = maps_in[b, size - 1, :, :dvv].astype(F32)
            for p in range(size - 2, -1, -1):
                made, last = piece(b, p)
                prod = mm(made[:, dvv:], both)
                both = last[:, :1] * both + made[:, :dvv].astype(F32) + prod
            bcomp[b] = both

        @pl.when((lag > 0) & (plane > 0))
        def _():
            made, g = piece(b, size - 1)
            both = made.astype(F32)
            for p in range(size - 2, -1, -1):
                made, last = piece(b, p)
                step = made.astype(F32)
                prod = mm(made[:, dvv:], both)
                both = last[:, :1] * both + jnp.concatenate(
                    [step[:, :dvv], g[:, :1] * step[:, dvv:]], axis=1
                ) + prod
                g = last * g
            bcomp[b] = both[:, :dvv]
            tcomp[b] = both[:, dvv:].astype(BF)
            gcomp[b] = jnp.broadcast_to(g, gcomp.shape[1:])

    def wait_plane(b):
        send_plane(b).wait_recv()

    def hand_on(b):
        @pl.when((lag == 0) & (plane > 0))
        def _():
            zout[b] = bcomp[b].astype(BF)

        @pl.when(lag > 0)
        def _():
            wait_plane(b)

            @pl.when(plane > 0)
            def _():
                eb = zin[b]
                e = gcomp[b, 0:1] * eb.astype(F32) + bcomp[b] + mm(tcomp[b], eb)
                zout[b] = e.astype(BF)

        @pl.when(plane > 0)
        def _():
            send_plane(b).start()

    def send_fars(b):
        i = b - chained

        @pl.when(lag == 0)
        def _():
            far_out[i, :dkk, :dvv] = bcomp[b].astype(BF)
            run(0, plane, lambda p: send_far(i, p, plane, offset_only).start())

        @pl.when(lag > 0)
        def _():
            g = gcomp[b]
            high = g.astype(BF)
            low = (g - high.astype(F32)).astype(BF)
            far_out[i, :dkk] = jnp.concatenate([bcomp[b].astype(BF), tcomp[b]], axis=1)
            far_out[i, dkk : dkk + 8, :dvv] = high
            far_out[i, dkk + 8 :, :dvv] = low
            run(0, plane, lambda p: send_far(i, p, plane, whole_map).start())

    def resolve(b):
        i = b - chained
        send_far(i, planes - 1, planes - 1, offset_only).wait_recv()

        def fold(d, e):
            source = planes - 2 - d
            send_far(i, source, source, whole_map).wait_recv()
            made = far_in[i, source, :dkk]
            g = far_in[i, source, dkk:, :dvv].astype(F32)
            prod = mm(made[:, dvv:], e)
            return (g[0:1] + g[8:9]) * e + made[:, :dvv].astype(F32) + prod

        e = far_in[i, planes - 1, :dkk, :dvv].astype(F32)
        zin[b] = lax.fori_loop(0, lag - 1, fold, e).astype(BF)

    def hand_back(b):
        eb = zin[b]
        e = eb.astype(F32)
        for p in range(size - 1, -1, -1):
            eout[b, p] = eb

            @pl.when(rank == p)
            def _():
                ein[rank * own + b] = eb

            @pl.when(rank != p)
            def _():
                send_back(b, p, rank).start()

            if p > 0:
                made, last = piece(b, p)
                e = last * e + made[:, :dvv].astype(F32) + mm(made[:, dvv:], eb)
                eb = e.astype(BF)

    def wait_back(b):
        for j in range(size):

            @pl.when(rank != j)
            def _():
                send_back(b, rank, j).wait_recv()

    def carry_batch(b):
        wait_back(b)
        parts = [
            carry_head(
                v[h], s0[h], ein[h], rows[h], kts[h], scales[h, 1:2], pairs[h], kks[h], ub[h],
                w0[h], nb[h], ks[h], dk0[h], dg0[h],
            )
            for h in batch_heads(b)
        ]
        outs = lockstep((parts, 1))[0]
        for j, h in enumerate(batch_heads(b)):
            dv[h] = outs[j][0].astype(BF)
            dk[h] = outs[j][1]
            dgs[pl.ds(h, 1), :] = outs[j][2]
            dbs[pl.ds(h, 1), :] = outs[j][3]

    late = max(own, planes) + 2


    def first_batch():
        local_batch(0)
        wait_barrier()
        run(1, m, lambda d: send_weights(side_ahead(d), side).start())
        end_sends()
        local_sends(0)

    def pass_on(s):
        turn = s - 1 - lag

        @pl.when((lag > 0) & (turn >= 0) & (turn < chained))
        def _():
            hand_on(turn)

        @pl.when((lag > 0) & (turn >= chained) & (turn < own))
        def _():
            resolve(turn)

    def gather_maps(s):
        @pl.when(s == 1)
        def _():
            wait_ends()

        compose(s - 1)

        @pl.when((lag == 0) & (s <= chained))
        def _():
            hand_on(s - 1)

        @pl.when((plane > 0) & (s > chained))
        def _():
            send_fars(s - 1)

    def early(s):
        both_batches(s)
        local_sends(s)
        pass_on(s)
        turn = jnp.where(lag == 0, s - 1, s)

        @pl.when(turn > 0)
        def _():
            gather_maps(turn)

    def middle():
        pass_on(own)
        rest_batch(own - 1)
        run(jnp.where(lag == 0, max(own - 1, 1), own), own + 1, gather_maps)
        run(0, jnp.maximum(own - lag, 0), hand_back)

    def later(s):
        pass_on(s)
        turn = s - 1 - lag

        @pl.when((turn >= 0) & (turn < own))
        def _():
            hand_back(turn)

        @pl.when(s >= late)
        def _():
            carry_batch(s - late)

    def take(first, last, pairs):
        for load in loads[first:last]:
            load.wait()
        for ref, raw in pairs:
            ref[...] = jnp.swapaxes(raw[...], 0, 1)

    take(0, 6, ())
    prepare()
    take(6, 9, ((k, k_raw), (q, q_raw), (do, do_raw)))
    first_batch()
    take(9, 11, ((v, v_raw),))
    run(1, own, early)
    middle()
    run(own + 1, own + late, later)

    def finish_grads():
        row, col = indices(c)
        tri = jnp.where(row >= col, 1.0, 0.0).astype(BF)
        sums = mm(jnp.concatenate(split3(dgs[...]), axis=0), tri)
        dlog = sums[:heads] + sums[heads : 2 * heads] + sums[2 * heads :]
        grads = jnp.concatenate([dlog * fac[:heads], dbs[...] * fac[heads:]], axis=0).astype(BF)
        ggot[side] = grads
        run(1, m, lambda d: send_grads(side_ahead(d), side).start())
        return grads

    def weight_terms(grads):
        terms = mm(grads, hidden[...])
        for i in range(adders):
            tbuf[i] = terms[:, i * w : (i + 1) * w].astype(BF)

        def give(to):
            @pl.when((to >= base) & (to < base + adders))
            def _():
                scatter(to - base, me).start()

        to_all(give)

    def partner(d):
        source = side_behind(d)
        send_weights(source, source).wait_recv()
        send_grads(source, source).wait_recv()

    def input_grad():
        wgot[side] = weights[side]
        run(1, m, partner)
        total = mm(ggot[0], wgot[0], 0, 0)
        for i in range(1, m):
            total = total + mm(ggot[i], wgot[i], 0, 0)
        gh[...] = total.astype(BF)

    def reduce_terms():
        def add(d, acc):
            source = behind(d)
            scatter(seat, source).wait_recv()
            return acc + got[source].astype(F32)

        @pl.when(adding)
        def _():
            acc = lax.fori_loop(1, n, add, tbuf[seat].astype(F32)).astype(BF)
            part[...] = acc
            gathered[seat] = acc
            to_all(lambda to: gather(to, seat).start())

    def arrivals():
        def arrive(i):
            @pl.when(i != seat)
            def _():
                gather(base, i).wait_recv()

        run(0, adders, arrive)

    def reorder():
        for ref, source in ((dq_out, dq), (dk_out, dk), (dv_out, dv)):
            ref[...] = jnp.swapaxes(source[...], 0, 1)

    def write_sums():
        for i in range(adders):
            both = gathered[i].astype(F32)
            gd[:, i * w : (i + 1) * w] = both[:heads]
            gw[:, i * w : (i + 1) * w] = both[heads:]

    def done(b):
        for j in range(size):

            @pl.when(rank != j)
            def _():
                send_map(b, j, rank).wait_send()
                send_back(b, j, rank).wait_send()

        @pl.when((plane > 0) & (b < chained))
        def _():
            send_plane(b).wait_send()

        @pl.when((b >= chained) & (lag == 0))
        def _():
            run(0, plane, lambda p: send_far(b - chained, p, plane, offset_only).wait_send())

        @pl.when((b >= chained) & (lag > 0))
        def _():
            run(0, plane, lambda p: send_far(b - chained, p, plane, whole_map).wait_send())

    weight_terms(finish_grads())
    input_grad()
    reduce_terms()
    reorder()
    arrivals()
    write_sums()
    for j in range(size):

        @pl.when(rank != j)
        def _():
            send_ends(j, rank).wait_send()

    run(0, own, done)
    def given(i):
        @pl.when(i != seat)
        def _():
            scatter(i, me).wait_send()

    run(0, adders, given)

    @pl.when(adding)
    def _():
        run(1, n, lambda d: gather(ahead(d), seat).wait_send())

    run(1, m, lambda d: send_weights(side_ahead(d), side).wait_send())
    run(1, m, lambda d: send_grads(side_ahead(d), side).wait_send())


def whole_part(n, m, q, k, v, do, s0, hidden, *gates):
    c, h, dk = q.shape
    dv = v.shape[2]
    size = group_size(n, h)
    own = h // size
    width = hidden.shape[1]
    adders = middle_planes(n // size)[1] * size
    w = width // adders
    vm = pl.BlockSpec(memory_space=pltpu.VMEM)
    sd = jax.ShapeDtypeStruct
    dma = pltpu.SemaphoreType.DMA
    message = (dk, dv + dk)
    return pl.pallas_call(
        partial(whole_kernel, n, m, size),
        out_shape=(
            pltpu.VMEM((c, h, dk), BF), pltpu.VMEM((c, h, dk), BF), pltpu.VMEM((c, h, dv), BF), pltpu.VMEM((c, width // m), BF),
            pltpu.VMEM((h, width), F32), pltpu.VMEM((h, width), F32),
        ),
        in_specs=[pl.BlockSpec(memory_space=pl.ANY)] * 11,
        out_specs=(vm,) * 6,
        scratch_shapes=[pltpu.VMEM(a.shape, a.dtype) for a in (q, k, v, do, s0, hidden) + gates]
        + [
            pltpu.VMEM((h, c, dk), BF), pltpu.VMEM((h, c, dk), BF), pltpu.VMEM((h, c, dv), BF),
            pltpu.VMEM((h, c, dv), BF),
            pltpu.VMEM((h, c, dk), BF), pltpu.VMEM((h, c, dk), BF), pltpu.VMEM((h, c, dv), BF),
            pltpu.VMEM((h, 8, c), F32), pltpu.VMEM((2 * h, c), F32),
            pltpu.VMEM((m, 2 * h, width // m), BF),
            pltpu.VMEM((h, dk, c), BF), pltpu.VMEM((h, dk, c), BF), pltpu.VMEM((h, 8, c), F32),
            pltpu.VMEM((h, c, c), F32), pltpu.VMEM((h, c, c), F32), pltpu.VMEM((h, c, c), F32),
            pltpu.VMEM((h, c, c), F32), pltpu.VMEM((h, c, c), BF), pltpu.VMEM((h, c, dv), F32),
            pltpu.VMEM((h, c, dk), BF), pltpu.VMEM((h, c, dv), F32), pltpu.VMEM((h, c, dv), BF),
            pltpu.VMEM((h, dk, c), F32),
            pltpu.VMEM((h, 1, c), F32), pltpu.VMEM((h, c), F32), pltpu.VMEM((h, c), F32),
            pltpu.VMEM((h, dv), F32), pltpu.VMEM((size, h, dv), F32),
            pltpu.VMEM((own, size) + message, BF), pltpu.VMEM((own, size) + message, BF),
            pltpu.VMEM((own, dk, dk), BF), pltpu.VMEM((own, dk, dv), F32),
            pltpu.VMEM((own, 8, dv), F32),
            pltpu.VMEM((min(own, 2), dk + 16, dv + dk), BF),
            pltpu.VMEM((min(own, 2), n // size, dk + 16, dv + dk), BF),
            pltpu.VMEM((own, dk, dv), BF), pltpu.VMEM((own, dk, dv), BF),
            pltpu.VMEM((own, size, dk, dv), BF), pltpu.VMEM((h, dk, dv), BF),
            pltpu.VMEM((adders, 2 * h, w), BF), pltpu.VMEM((n, 2 * h, w), BF),
            pltpu.VMEM((2 * h, w), BF), pltpu.VMEM((adders, 2 * h, w), BF),
            pltpu.VMEM((m, 2 * h, c), BF), pltpu.VMEM((m, 2 * h, width // m), BF),
            dma((11,)), dma((2, min(own, 2), n // size)), dma((2, size)), dma((own, size)), dma((own, size)), dma((2, own)), dma((own, size)), dma((h,)),
            dma((4, n)), dma((4, m)),
        ],
        compiler_params=pltpu.CompilerParams(
            collective_id=0, has_side_effects=True, vmem_limit_bytes=57000 * 1024
        ),
    )(q, k, v, do, s0, hidden, *gates)


def store_kernel(*refs):
    count = (len(refs) - 1) // 2
    sems = refs[-1]
    copies = [
        pltpu.make_async_copy(refs[i], refs[count + i], sems.at[i]) for i in range(count)
    ]
    for copy in copies:
        copy.start()
    for copy in copies:
        copy.wait()


def store_part(arrays):
    count = len(arrays)
    return pl.pallas_call(
        store_kernel,
        out_shape=tuple(jax.ShapeDtypeStruct(a.shape, a.dtype) for a in arrays),
        in_specs=[pl.BlockSpec(memory_space=pltpu.VMEM)] * count,
        out_specs=(pl.BlockSpec(memory_space=pl.ANY),) * count,
        scratch_shapes=[pltpu.SemaphoreType.DMA((count,))],
        compiler_params=pltpu.CompilerParams(vmem_limit_bytes=8 * 1024 * 1024),
    )(*arrays)


def shards(
    queries,
    key_vectors,
    values,
    out_grad,
    hidden_in,
    decay_weight,
    write_weight,
    decay_bias,
    decay_log,
    write_bias,
    start_state,
):
    n, m = lax.axis_size("seq"), lax.axis_size("head")
    made = whole_part(
        n, m, queries, key_vectors, values, out_grad, start_state[0], hidden_in, decay_weight.T, write_weight.T,
        decay_bias[None], decay_log[None], write_bias[None],
    )
    dq, dk, dv, gh, gd, gw = store_part(made)
    return dq, dk, dv, gh, gd.T, gw.T


def solution(mesh):
    placed = (
        P("seq", "head", None),
        P("seq", "head", None),
        P("seq", "head", None),
        P("seq", "head", None),
        P("seq", None),
        P(None, "head"),
        P(None, "head"),
        P("head"),
        P("head"),
        P("head"),
        P("seq", "head", None, None),
    )
    return jax.shard_map(
        shards,
        mesh=mesh,
        in_specs=placed,
        out_specs=(
            P("seq", "head", None),
            P("seq", "head", None),
            P("seq", "head", None),
            P("seq", "head"),
            P(None, "head"),
            P(None, "head"),
        ),
        check_vma=False,
    )
```
